32 devices in a mesh: etp: 4 (over z), ep: 8 (over y, x, core).
Axes of the slice: x: 2, y: 2, z: 4, core: 2. Of those that a mesh axis runs over, the one named last changes fastest.
Arguments:
- hidden: bfloat16 [16384, 1024], P(('ep', 'etp'))
- w_router: float32 [1024, 8], replicated
- expert_ids: int32 [16384, 2], P(('ep', 'etp'))
- d_out: bfloat16 [16384, 1024], P(('ep', 'etp'))
- w_gate: bfloat16 [8, 1024, 7168], P('ep', None, 'etp')
- w_up: bfloat16 [8, 1024, 7168], P('ep', None, 'etp')
- w_down: bfloat16 [8, 7168, 1024], P('ep', 'etp')
Outputs:
- output 1: bfloat16 [16384, 1024], P(('ep', 'etp'))
- output 2: bfloat16 [16384, 1024], P(('ep', 'etp'))
- output 3: float32 [1024, 8], replicated
- output 4: float32 [], replicated
- output 5: float32 [8, 1024, 7168], P('ep', None, 'etp')
- output 6: float32 [8, 1024, 7168], P('ep', None, 'etp')
- output 7: float32 [8, 7168, 1024], P('ep', 'etp')
All inputs are finite; a program needn't handle non-finite values.
Results may differ from the reference program's by a relative error of at most 0.00896172.
Values are sent between devices in bfloat16 or wider.
A program may use at most 1 GiB of HBM per device.

```python
import jax
import jax.numpy as jnp
from jax import lax

EXPERTS = 8
D_MODEL = 1024
D_FF = 7168
TOKENS = 16384
N_DEVICES = 32

CAPACITY = (5 * TOKENS + 2 * EXPERTS - 1) // (2 * EXPERTS)
BLOCK_TOKENS = TOKENS // N_DEVICES


def draw_choices(draw_key):
    quarter = BLOCK_TOKENS // (2 * EXPERTS)
    perm_key, block_key = jax.random.split(draw_key)
    expert_order = jax.random.permutation(perm_key, EXPERTS)
    hot_shift = jnp.zeros((EXPERTS,), jnp.int32).at[:4].set(jnp.array([2, 2, -2, -2], jnp.int32) * quarter)

    def one_block(one_key):
        k_noise, k_rows, k_flip = jax.random.split(one_key, 3)
        count_noise = jax.random.randint(k_noise, (EXPERTS,), 0, quarter + 1)
        count_noise = count_noise.at[0].set(quarter).at[1].set(0)
        count_perm = 4 * quarter + count_noise - jnp.roll(count_noise, -1) + hot_shift
        counts = jnp.zeros((EXPERTS,), jnp.int32).at[expert_order].set(count_perm)
        ends = jnp.cumsum(counts)
        id_seq = jnp.sum(jnp.arange(2 * BLOCK_TOKENS)[:, None] >= ends[None, :], axis=1).astype(jnp.int32)
        id_pairs = jnp.stack([id_seq[:BLOCK_TOKENS], id_seq[BLOCK_TOKENS:]], axis=1)
        id_pairs = id_pairs[jax.random.permutation(k_rows, BLOCK_TOKENS)]
        flip_mask = jax.random.randint(k_flip, (BLOCK_TOKENS, 1), 0, 2) == 1
        return jnp.where(flip_mask, id_pairs[:, ::-1], id_pairs)

    blocks = jax.vmap(one_block)(jax.random.split(block_key, N_DEVICES))
    return blocks.reshape(TOKENS, 2)


def setup_inputs(seed: int = 0) -> dict:
    root_key = jax.random.key(seed)
    k_hid, k_route, k_ids, k_dout, k_gate, k_up, k_down = jax.random.split(root_key, 7)
    hidden = jax.random.normal(k_hid, (TOKENS, D_MODEL), jnp.float32).astype(jnp.bfloat16)
    w_router = jax.random.normal(k_route, (D_MODEL, EXPERTS), jnp.float32) * (0.5 * D_MODEL ** -0.5)
    expert_ids = draw_choices(k_ids)
    d_out = jax.random.normal(k_dout, (TOKENS, D_MODEL), jnp.float32).astype(jnp.bfloat16)
    w_gate = (jax.random.normal(k_gate, (EXPERTS, D_MODEL, D_FF), jnp.float32) * D_MODEL ** -0.5).astype(jnp.bfloat16)
    w_up = (jax.random.normal(k_up, (EXPERTS, D_MODEL, D_FF), jnp.float32) * D_MODEL ** -0.5).astype(jnp.bfloat16)
    w_down = (jax.random.normal(k_down, (EXPERTS, D_FF, D_MODEL), jnp.float32) * D_FF ** -0.5).astype(jnp.bfloat16)
    return {"hidden": hidden, "w_router": w_router, "expert_ids": expert_ids, "d_out": d_out, "w_gate": w_gate, "w_up": w_up, "w_down": w_down}


def route_terms(logits, expert_ids):
    prob_vals = jax.nn.softmax(logits, axis=-1)
    picked = jnp.take_along_axis(prob_vals, expert_ids, axis=1)
    return picked / jnp.sum(picked, axis=1, keepdims=True), jnp.sum(prob_vals, axis=0)


def expert_pass(operands):
    x_buf, dy_buf, gate_w, up_w, down_w = operands
    act_a = jnp.dot(x_buf, gate_w, preferred_element_type=jnp.float32)
    act_b = jnp.dot(x_buf, up_w, preferred_element_type=jnp.float32)
    sig_a = jax.nn.sigmoid(act_a)
    silu_a = act_a * sig_a
    inner_act = (silu_a * act_b).astype(jnp.bfloat16)
    y_buf = jnp.dot(inner_act, down_w, preferred_element_type=jnp.float32).astype(jnp.bfloat16)
    d_inner = jnp.dot(dy_buf, down_w.T, preferred_element_type=jnp.float32)
    d_act_a = (d_inner * act_b * sig_a * (1.0 + act_a * (1.0 - sig_a))).astype(jnp.bfloat16)
    d_act_b = (d_inner * silu_a).astype(jnp.bfloat16)
    dx_buf = (jnp.dot(d_act_a, gate_w.T, preferred_element_type=jnp.float32) + jnp.dot(d_act_b, up_w.T, preferred_element_type=jnp.float32)).astype(jnp.bfloat16)
    g_gate = jnp.dot(x_buf.T, d_act_a, preferred_element_type=jnp.float32)
    g_up = jnp.dot(x_buf.T, d_act_b, preferred_element_type=jnp.float32)
    g_down = jnp.dot(inner_act.T, dy_buf, preferred_element_type=jnp.float32)
    return y_buf, dx_buf, g_gate, g_up, g_down


def reference(hidden, w_router, expert_ids, d_out, w_gate, w_up, w_down):
    hidden_f = hidden.astype(jnp.float32)
    logits = jnp.dot(hidden_f, w_router, preferred_element_type=jnp.float32)
    (gate_vals, prob_sum), route_vjp = jax.vjp(lambda logit_in: route_terms(logit_in, expert_ids), logits)
    n_assign = 2 * TOKENS
    flat_ids = expert_ids.reshape(-1)
    assign = jnp.arange(n_assign, dtype=jnp.int32)
    counts = jnp.bincount(flat_ids, length=EXPERTS)
    sort_order = jnp.argsort(flat_ids * n_assign + assign)
    sort_rank = jnp.zeros((n_assign,), jnp.int32).at[sort_order].set(assign)
    starts = jnp.cumsum(counts) - counts
    slot_pos = sort_rank - starts[flat_ids]
    dest_rows = jnp.where(slot_pos < CAPACITY, flat_ids * CAPACITY + slot_pos, EXPERTS * CAPACITY)
    source = jnp.full((EXPERTS * CAPACITY,), n_assign, jnp.int32).at[dest_rows].set(assign, mode="drop")
    x_buf = jnp.take(hidden, source // 2, axis=0, mode="fill", fill_value=0).reshape(EXPERTS, CAPACITY, D_MODEL)
    d_mix = 2.0 * d_out.astype(jnp.float32)
    dy_assign = (gate_vals[:, :, None] * d_mix[:, None, :]).astype(jnp.bfloat16).reshape(n_assign, D_MODEL)
    dy_buf = jnp.take(dy_assign, source, axis=0, mode="fill", fill_value=0).reshape(EXPERTS, CAPACITY, D_MODEL)
    y_buf, dx_buf, g_gate, g_up, g_down = lax.map(expert_pass, (x_buf, dy_buf, w_gate, w_up, w_down))
    y_pair = jnp.take(y_buf.reshape(EXPERTS * CAPACITY, D_MODEL), dest_rows, axis=0, mode="fill", fill_value=0).reshape(TOKENS, 2, D_MODEL).astype(jnp.float32)
    dx_pair = jnp.take(dx_buf.reshape(EXPERTS * CAPACITY, D_MODEL), dest_rows, axis=0, mode="fill", fill_value=0).reshape(TOKENS, 2, D_MODEL).astype(jnp.float32)
    output = (hidden_f + 2.0 * jnp.sum(gate_vals[:, :, None] * y_pair, axis=1)).astype(jnp.bfloat16)
    d_gates = jnp.sum(d_mix[:, None, :] * y_pair, axis=2)
    route_frac = counts.astype(jnp.float32) / n_assign
    aux_loss = 0.01 * EXPERTS * jnp.sum(route_frac * prob_sum) / TOKENS
    (d_logits,) = route_vjp((d_gates, (0.01 * EXPERTS / TOKENS) * route_frac))
    d_router = jnp.dot(hidden_f.T, d_logits, preferred_element_type=jnp.float32)
    d_hidden = (d_out.astype(jnp.float32) + jnp.sum(dx_pair, axis=1) + jnp.dot(d_logits, w_router.T, preferred_element_type=jnp.float32)).astype(jnp.bfloat16)
    return output, d_hidden, d_router, aux_loss, g_gate, g_up, g_down
```

```python
import functools
import jax
import jax.numpy as jnp
from jax import lax
from jax.experimental import pallas as pl
from jax.experimental.pallas import tpu as pltpu
from jax.sharding import PartitionSpec as P


AUX_COEF = 0.01
OUT_SCALE = 2.0
ALL_AXES = ("ep", "etp")
BF16 = jnp.bfloat16
F32 = jnp.float32
MIB = 1 << 20
FF_STEP = 256

NEXT_PAIRS = (1, 0, 3, 2)
ENDS_PAIRS = (3, 2, 1, 0)


def mm(lhs, rhs):
    return jnp.dot(lhs, rhs, preferred_element_type=F32)


def mm_nt(lhs, rhs):
    return lax.dot_general(lhs, rhs, (((1,), (1,)), ((), ())), preferred_element_type=F32)


def mm_tn(lhs, rhs):
    return lax.dot_general(lhs, rhs, (((0,), (0,)), ((), ())), preferred_element_type=F32)


def params(vmem_mib, dims=1):
    return pltpu.CompilerParams(dimension_semantics=("arbitrary",) * dims, vmem_limit_bytes=vmem_mib * MIB)


def pick_kernel(scaled, win, planes_ref, slots_ref, base_ref, src_ref, pos_ref, *rest):
    if scaled:
        gate_ref, out_ref, acc_ref = rest
    else:
        out_ref, acc_ref = rest
    grp = pl.program_id(0)
    blk = pl.program_id(1)

    @pl.when(blk == 0)
    def _():
        acc_ref[...] = jnp.zeros_like(acc_ref)

    base = pl.multiple_of(base_ref[grp, blk], 8)
    pos_row = pos_ref[0]
    want = base + lax.broadcasted_iota(jnp.int32, (win, pos_row.shape[1]), 0)
    hit = want == pos_row
    part = mm(hit.astype(F32).astype(BF16), src_ref[0])
    if scaled:
        part = part * jnp.sum(jnp.where(hit, gate_ref[0], 0.0), axis=1, keepdims=True)
    acc_ref[pl.ds(base, win), :] += part

    @pl.when(blk == pl.num_programs(1) - 1)
    def _():
        out_ref[...] = acc_ref[: out_ref.shape[0], :].astype(out_ref.dtype)


def pick_rows(source, pos, gates, planes, slots, base, n_rows, win, n_src, n_etp):
    blk_rows = pos.shape[-1]
    d_model = source.shape[2]
    n_grp = planes.shape[0]
    src_map = lambda g, o, planes, slots, base: (o * n_etp + slots[g], 0, 0)
    tab_map = lambda g, o, planes, slots, base: (o * n_etp + planes[g], 0, 0)
    in_specs = [pl.BlockSpec((1, blk_rows, d_model), src_map), pl.BlockSpec((1, 1, blk_rows), tab_map)]
    operands = [source, pos[:, None, :]]
    if gates is not None:
        in_specs.append(pl.BlockSpec((1, 1, blk_rows), tab_map))
        operands.append(gates[:, None, :])
    flops = 2 * n_grp * n_src * win * blk_rows * d_model
    return pl.pallas_call(
        functools.partial(pick_kernel, gates is not None, win),
        grid_spec=pltpu.PrefetchScalarGridSpec(
            num_scalar_prefetch=3,
            grid=(n_grp, n_src),
            in_specs=in_specs,
            out_specs=pl.BlockSpec((n_rows, d_model), lambda g, o, planes, slots, base: (g, 0)),
            scratch_shapes=[pltpu.VMEM((n_rows + win, d_model), F32)],
        ),
        out_shape=jax.ShapeDtypeStruct((n_grp * n_rows, d_model), BF16),
        compiler_params=params(32, 2),
        cost_estimate=pl.CostEstimate(flops=flops, bytes_accessed=2 * source.size * 2, transcendentals=0),
        name="pick_rows",
    )(planes, slots, base, *operands)


def whole(array):
    return pl.BlockSpec(array.shape, lambda i: (0, 0), pipeline_mode=pl.Buffered(1))


def fwd_kernel(n_sets, x_ref, *refs):
    weights, (*base_ref, y_ref, u_ref) = refs[: 3 * n_sets], refs[3 * n_sets :]
    for s in range(n_sets):
        w1, w3, w2 = weights[3 * s : 3 * s + 3]

        def step(i, _):
            cols = pl.ds(pl.multiple_of(i * FF_STEP, FF_STEP), FF_STEP)
            act_a = mm(x_ref[...], w1[:, cols])
            act_b = mm(x_ref[...], w3[:, cols])
            u_ref[:, cols] = (act_a * jax.nn.sigmoid(act_a) * act_b).astype(BF16)
            return 0

        lax.fori_loop(0, w1.shape[1] // FF_STEP, step, 0)
        part = mm(u_ref[...], w2[...])
        if s > 0:
            y_ref[...] += part
        elif base_ref:
            y_ref[...] = base_ref[0][...] + part
        else:
            y_ref[...] = part


def ffn_fwd(x, sets, tile, first, n_tiles, base=()):
    d_model, d_ff = sets[0].shape
    rows = n_tiles * tile
    n_sets = len(sets) // 3
    return pl.pallas_call(
        functools.partial(fwd_kernel, n_sets),
        grid=(n_tiles,),
        in_specs=[pl.BlockSpec((tile, d_model), lambda i: (i + first, 0))] + [whole(w) for w in sets] + [pl.BlockSpec((tile, d_model), lambda i: (i + first, 0))] * len(base),
        out_specs=pl.BlockSpec((tile, d_model), lambda i: (i, 0)),
        out_shape=jax.ShapeDtypeStruct((rows, d_model), F32),
        scratch_shapes=[pltpu.VMEM((tile, d_ff), BF16)],
        compiler_params=params(56),
        cost_estimate=pl.CostEstimate(flops=6 * rows * d_model * d_ff * n_sets, bytes_accessed=6 * d_model * d_ff * n_sets + 6 * rows * d_model, transcendentals=rows * d_ff * n_sets),
        name="ffn_fwd",
    )(x, *sets, *base)


def bwd_kernel(n_sets, with_dx, with_y, n_alias, x_ref, c_ref, *refs):
    weights, refs = refs[: 3 * n_sets], list(refs[3 * n_sets + n_alias :])
    u_ref, da_ref, db_ref = refs[:3]
    dx_ref = refs.pop(3) if with_dx else None
    y_ref = refs.pop(3) if with_y else None
    tmp = refs[3:]
    for s in range(n_sets):
        w1, w3, w2 = weights[3 * s : 3 * s + 3]
        da, db, u = (da_ref, db_ref, u_ref) if s == 0 else (tmp[0], tmp[1], tmp[-1])
        with_u = s == 0 or with_y

        def step(i, _):
            cols = pl.ds(pl.multiple_of(i * FF_STEP, FF_STEP), FF_STEP)
            act_a = mm(x_ref[...], w1[:, cols])
            act_b = mm(x_ref[...], w3[:, cols])
            d_inner = mm_nt(c_ref[...], w2[cols, :])
            sig_a = jax.nn.sigmoid(act_a)
            silu_a = act_a * sig_a
            if with_u:
                u[:, cols] = (silu_a * act_b).astype(BF16)
            da[:, cols] = (d_inner * act_b * sig_a * (1.0 + act_a * (1.0 - sig_a))).astype(BF16)
            db[:, cols] = (d_inner * silu_a).astype(BF16)
            return 0

        lax.fori_loop(0, w1.shape[1] // FF_STEP, step, 0)
        if with_dx:
            part = mm_nt(da[...], w1[...]) + mm_nt(db[...], w3[...])
            if s == 0:
                dx_ref[...] = part
            else:
                dx_ref[...] += part
        if with_y:
            part = mm(u[...], w2[...])
            if s == 0:
                y_ref[...] = part
            else:
                y_ref[...] += part


def ffn_bwd(x, c, sets, tile, first, n_tiles, kept, with_dx=True, with_y=False):
    d_model, d_ff = sets[0].shape
    rows = n_tiles * tile
    n_sets = len(sets) // 3
    row_in = pl.BlockSpec((tile, d_model), lambda i: (i + first, 0))
    out_specs = [pl.BlockSpec((tile, d_ff), lambda i: (i + first, 0))] * 3
    out_shape = [jax.ShapeDtypeStruct((x.shape[0], d_ff), BF16)] * 3
    n_sums = int(with_dx) + int(with_y)
    out_specs += [pl.BlockSpec((tile, d_model), lambda i: (i, 0))] * n_sums
    out_shape += [jax.ShapeDtypeStruct((rows, d_model), F32)] * n_sums
    scratch = [pltpu.VMEM((tile, d_ff), BF16)] * (3 if with_y else 2) if n_sets > 1 else []
    n_in = 2 + len(sets)
    return pl.pallas_call(
        functools.partial(bwd_kernel, n_sets, with_dx, with_y, len(kept)),
        grid=(n_tiles,),
        in_specs=[row_in, row_in] + [whole(w) for w in sets] + [pl.BlockSpec(memory_space=pl.ANY)] * len(kept),
        out_specs=out_specs,
        out_shape=out_shape,
        scratch_shapes=scratch,
        input_output_aliases={n_in + i: i for i in range(len(kept))},
        compiler_params=params(60),
        cost_estimate=pl.CostEstimate(flops=(6 + 4 * with_dx + 2 * with_y) * rows * d_model * d_ff * n_sets, bytes_accessed=6 * d_model * d_ff * n_sets + 8 * rows * (d_model + d_ff), transcendentals=rows * d_ff * n_sets),
        name="ffn_bwd",
    )(x, c, *sets, *kept)


def home_kernel(win, n_far, start_ref, near_ref, *refs):
    fars, (more_ref, out_ref, sum_ref) = refs[:n_far], refs[n_far:]
    row = 0
    for far in fars:
        rows = far.shape[0]
        sum_ref[row : row + rows, :] = (near_ref[row : row + rows, :] + far[...]).astype(BF16).astype(F32)
        row += rows
    sum_ref[row : row + more_ref.shape[0], :] = more_ref[...].astype(F32)
    row += more_ref.shape[0]
    sum_ref[row:, :] = jnp.zeros((sum_ref.shape[0] - row, sum_ref.shape[1]), F32)
    out_rows = out_ref.shape[1]
    to = lax.broadcasted_iota(jnp.int32, (out_rows, win), 0)
    frm = lax.broadcasted_iota(jnp.int32, (out_rows, win), 1)
    for o in range(out_ref.shape[0]):
        start = start_ref[o]
        base = pl.multiple_of(start // 8 * 8, 8)
        rows = sum_ref[pl.ds(base, win), :].astype(BF16)
        move = (frm == to + (start - base)).astype(F32).astype(BF16)
        out_ref[o] = mm(move, rows).astype(BF16)


def home_blocks(starts, near, fars, more, out_rows):
    n_out = starts.shape[0]
    d_model = near.shape[1]
    win = out_rows + 8
    vmem = pl.BlockSpec(memory_space=pltpu.VMEM)
    return pl.pallas_call(
        functools.partial(home_kernel, win, len(fars)),
        in_specs=[pl.BlockSpec(memory_space=pltpu.SMEM)] + [vmem] * (2 + len(fars)),
        out_specs=vmem,
        out_shape=jax.ShapeDtypeStruct((n_out, out_rows, d_model), BF16),
        scratch_shapes=[pltpu.VMEM((near.shape[0] + more.shape[0] + win, d_model), F32)],
        compiler_params=pltpu.CompilerParams(vmem_limit_bytes=40 * MIB),
        cost_estimate=pl.CostEstimate(flops=2 * n_out * out_rows * win * d_model, bytes_accessed=12 * near.size, transcendentals=0),
        name="home_blocks",
    )(starts, near, *fars, more)


def split3(value):
    high = lax.reduce_precision(value, 8, 7)
    rest = value - high
    mid = lax.reduce_precision(rest, 8, 7)
    return high.astype(BF16), mid.astype(BF16), (rest - mid).astype(BF16)


def solution(mesh):
    ep_size = mesh.shape["ep"]
    etp_size = mesh.shape["etp"]
    n_dev = ep_size * etp_size
    tok_spec = P(ALL_AXES, None)
    gate_spec = P("ep", None, "etp")
    down_spec = P("ep", "etp", None)

    def layer(hidden, w_router, expert_ids, d_out, w_gate, w_up, w_down):
        tok_rows, d_model = hidden.shape
        n_experts = w_router.shape[1]
        n_tokens = tok_rows * n_dev
        capacity = (5 * n_tokens + 2 * n_experts - 1) // (2 * n_experts)
        per_expert = 7 * tok_rows // (2 * n_experts)
        list_max = ep_size * per_expert
        main_rows = 23 * tok_rows // 8
        more_rows = list_max - main_rows
        tile = main_rows // 2
        win = per_expert + 8
        ep_i = lax.axis_index("ep")
        etp_i = lax.axis_index("etp")
        block_idx = ep_i * etp_size + etp_i
        w1, w3, w2 = w_gate[0], w_up[0], w_down[0]

        def swap(array, even, odd):
            pairs = [(t * ep_size + o, (odd if o % 2 else even)[t] * ep_size + o) for t in range(etp_size) for o in range(ep_size)]
            return lax.ppermute(array, ("etp", "ep"), pairs)

        def spread(array):
            shifts = range(1, etp_size)
            moved = [lax.ppermute(array, "etp", [(t, (t + k) % etp_size) for t in range(etp_size)]) for k in shifts]
            return [array] + moved

        ids_row = expert_ids.T.astype(BF16).reshape(1, 2 * tok_rows)
        ids_row = jnp.concatenate([ids_row, jnp.zeros((7, 2 * tok_rows), BF16)])
        h_col = lax.all_gather(jnp.concatenate([hidden, ids_row]), "etp")
        w1_b, w3_b, w2_b, dy_b, h_col = lax.optimization_barrier((w1, w3, w2, d_out, h_col))
        dy_parts = spread(dy_b)
        w1p, w3p, w2p = [swap(w, NEXT_PAIRS, ENDS_PAIRS) for w in (w1_b, w3_b, w2_b)]
        h_all = lax.all_gather(h_col, "ep").reshape(n_dev, tok_rows + 8, d_model)
        *dy_parts, h_all = lax.optimization_barrier((*dy_parts, h_all))
        dy_col = jnp.stack(dy_parts)
        dy_all = lax.all_gather(dy_col, "ep").reshape(n_dev, tok_rows, d_model)

        ids_all = h_all[:, tok_rows, :].astype(jnp.int32).reshape(n_dev, 2, tok_rows)
        id0, id1 = ids_all[:, 0], ids_all[:, 1]
        experts = jnp.arange(n_experts, dtype=jnp.int32)[None, :, None]
        count = jnp.sum(((id0[:, None, :] == experts) | (id1[:, None, :] == experts)).astype(F32), axis=2)
        before = jnp.cumsum(count, axis=0) - count
        kept = jnp.clip(capacity - before, 0, count).astype(jnp.int32)
        kept_lists = kept.reshape(ep_size, etp_size, n_experts)
        list_start = jnp.cumsum(kept_lists, axis=0) - kept_lists
        list_len = jnp.sum(kept_lists, axis=0)
        earlier = (jnp.arange(tok_rows)[:, None] < jnp.arange(tok_rows)[None, :]).astype(BF16)

        my_member = (id0 == ep_i) | (id1 == ep_i)
        my_rank = mm(my_member.astype(BF16), earlier).astype(jnp.int32)
        my_start = lax.dynamic_index_in_dim(list_start, ep_i, 2, keepdims=False)
        my_kept = lax.dynamic_index_in_dim(kept, ep_i, 1, keepdims=True)
        my_pos = jnp.where(my_member & (my_rank < my_kept), my_start.reshape(n_dev, 1) + my_rank, -1)
        odd = ep_i % 2
        far = jnp.where(odd == 1, etp_i ^ 1, etp_size - 1 - etp_i)
        planes = jnp.stack([far, etp_i, far ^ 2, etp_i ^ 2]).astype(jnp.int32)
        my_base = jnp.minimum(my_start, main_rows) // 8 * 8
        pick = functools.partial(pick_rows, win=win, n_src=ep_size, n_etp=etp_size)
        main_pos = jnp.where(my_pos < main_rows, my_pos, -1)
        main_base = my_base.T[planes]
        dy_slots = (etp_i - planes) % etp_size
        x_main = pick(h_all, main_pos, None, planes, planes, main_base, main_rows)

        route_w = jnp.concatenate(split3(w_router), axis=1)
        logit_parts = lax.dot_general(route_w, h_all, (((0,), (2,)), ((), ())), preferred_element_type=F32)[:, :, :tok_rows].reshape(-1, n_tokens)
        logits = logit_parts[:n_experts] + logit_parts[n_experts : 2 * n_experts] + logit_parts[2 * n_experts :]
        probs_all = jax.nn.softmax(logits, axis=0)
        expert_col = jnp.arange(n_experts, dtype=jnp.int32)[:, None]
        picked_all = jnp.where((id0.reshape(1, -1) == expert_col) | (id1.reshape(1, -1) == expert_col), probs_all, 0.0)
        my_gate = lax.dynamic_index_in_dim(picked_all, ep_i, 0, keepdims=False) / jnp.sum(picked_all, axis=0)
        mean_prob = jnp.sum(probs_all, axis=1) / n_tokens
        my_scale = OUT_SCALE * my_gate.reshape(n_dev, tok_rows)
        c_main = pick(dy_all, main_pos, my_scale, planes, dy_slots, main_base, main_rows)

        own, pair = (w1, w3, w2), (w1p, w3p, w2p)
        y_base = ffn_fwd(x_main, own, tile, 0, 2)
        y_far = []
        for i in range(2):
            y_part = ffn_fwd(x_main, pair, tile, i, 1, (y_base,))
            y_far.append(swap(y_part, ENDS_PAIRS, NEXT_PAIRS))
        dx_far, acts = [], ()
        for i in range(2):
            *acts, dx_part = ffn_bwd(x_main, c_main, own + pair, tile, i, 1, acts)
            dx_far.append(swap(dx_part, ENDS_PAIRS, NEXT_PAIRS))
        *acts, dx_near, y_near = ffn_bwd(x_main, c_main, own + pair, tile // 2, 4, 4, acts, with_y=True)
        inner, d_a, d_b = ffn_bwd(x_main, c_main, own, tile, 4, 4, acts, with_dx=False)

        def more_work():
            more_pos = jnp.where(my_pos >= main_rows, my_pos - main_rows, -1)
            more_base = jnp.clip(my_start.T - main_rows, 0, more_rows) // 8 * 8
            order = jnp.arange(etp_size, dtype=jnp.int32)
            x_more = pick(h_all, more_pos, None, order, order, more_base, more_rows)
            c_more = pick(dy_all, more_pos, my_scale, order, (etp_i - order) % etp_size, more_base, more_rows)
            inner, d_a, d_b, dx_part, y_part = ffn_bwd(x_more, c_more, own, more_rows, 0, etp_size, (), with_y=True)
            y_more = lax.psum_scatter(y_part, "etp", scatter_dimension=0, tiled=True)
            dx_more = lax.psum_scatter(dx_part, "etp", scatter_dimension=0, tiled=True)
            return y_more.astype(BF16), dx_more.astype(BF16), x_more, c_more, inner, d_a, d_b

        def no_more_work():
            none = jnp.zeros((more_rows, d_model), BF16)
            rows = jnp.zeros((etp_size * more_rows, d_model), BF16)
            acts = jnp.zeros((etp_size * more_rows, w1.shape[1]), BF16)
            return none, none, rows, rows, acts, acts, acts

        any_more = jnp.max(list_len) > main_rows
        y_more, dx_more, *more = lax.cond(any_more, more_work, no_more_work)

        home_start = lax.dynamic_index_in_dim(my_start, etp_i, 1, keepdims=False)

        def send_home(near, fars, more):
            blocks = home_blocks(home_start, near, fars, more, per_expert)
            return lax.all_to_all(blocks, "ep", 0, 0, tiled=True).reshape(n_experts * per_expert, d_model)

        hot = [(expert_ids[:, k : k + 1] == experts[0].T).astype(F32) for k in range(2)]
        probs = lax.dynamic_slice_in_dim(probs_all, block_idx * tok_rows, tok_rows, 1).T
        picked = [jnp.sum(probs * hot[k], axis=1, keepdims=True) for k in range(2)]
        pick_sum = picked[0] + picked[1]
        gates = [picked[k] / pick_sum for k in range(2)]
        my_kept_row = lax.dynamic_index_in_dim(kept, block_idx, 0, keepdims=True).astype(F32)
        rank = mm_tn(earlier, (hot[0] + hot[1]).astype(BF16))
        slot_row = jnp.arange(n_experts * per_expert, dtype=jnp.int32)[None, :]
        chosen = []
        for k in range(2):
            rank_k = jnp.sum(rank * hot[k], axis=1, keepdims=True)
            kept_k = jnp.sum(my_kept_row * hot[k], axis=1, keepdims=True)
            slot_k = jnp.where(rank_k < kept_k, expert_ids[:, k : k + 1] * per_expert + rank_k.astype(jnp.int32), -1)
            chosen.append(slot_k == slot_row)

        y_back = send_home(y_near, y_far, y_more)
        y_pair = [mm(chosen[k].astype(BF16), y_back) for k in range(2)]
        hidden_f = hidden.astype(F32)
        output = (hidden_f + OUT_SCALE * (gates[0] * y_pair[0] + gates[1] * y_pair[1])).astype(BF16)
        d_out_f = d_out.astype(F32)
        d_gates = [jnp.sum(OUT_SCALE * d_out_f * y_pair[k], axis=1, keepdims=True) for k in range(2)]

        route_frac = jnp.sum(count, axis=0) / (2 * n_tokens)
        aux_loss = AUX_COEF * n_experts * jnp.sum(route_frac * mean_prob)
        mix = gates[0] * d_gates[0] + gates[1] * d_gates[1]
        d_probs = (AUX_COEF * n_experts / n_tokens) * route_frac[None, :]
        for k in range(2):
            d_probs = d_probs + hot[k] * ((d_gates[k] - mix) / pick_sum)
        d_logits = probs * (d_probs - jnp.sum(probs * d_probs, axis=1, keepdims=True))
        d_router_part = lax.dot_general(d_logits, hidden_f, (((0,), (0,)), ((), ())), precision=lax.Precision.HIGHEST, preferred_element_type=F32)
        x_main, c_main, inner, d_router_part = lax.optimization_barrier((x_main, c_main, inner, d_router_part))
        d_router = jnp.sum(lax.all_gather(d_router_part, ALL_AXES), axis=0).T
        dw1 = mm_tn(x_main, d_a)
        dw3 = mm_tn(x_main, d_b)
        dx_near, dw1, dw3 = lax.optimization_barrier((dx_near, dw1, dw3))
        dx_back = send_home(dx_near, dx_far, dx_more)
        dw2 = mm_tn(inner, c_main)

        def add_more(*grads):
            x_more, c_more, inner_more, d_a_more, d_b_more = more
            return grads[0] + mm_tn(x_more, d_a_more), grads[1] + mm_tn(x_more, d_b_more), grads[2] + mm_tn(inner_more, c_more)

        dw1, dw3, dw2 = lax.cond(any_more, add_more, lambda *grads: grads, dw1, dw3, dw2)
        d_route = lax.dot_general(d_logits, w_router, (((1,), (1,)), ((), ())), precision=lax.Precision.HIGHEST, preferred_element_type=F32)
        dx_sum = mm((chosen[0] | chosen[1]).astype(BF16), dx_back)
        d_hidden = (d_out_f + dx_sum + d_route).astype(BF16)
        return output, d_hidden, d_router, aux_loss, dw1[None], dw3[None], dw2[None]

    return jax.shard_map(layer, mesh=mesh, in_specs=(tok_spec, P(), tok_spec, tok_spec, gate_spec, gate_spec, down_spec), out_specs=(tok_spec, tok_spec, P(), P(), gate_spec, gate_spec, down_spec), check_vma=False)
```

```python
import functools
import jax
import jax.numpy as jnp
from jax import lax
from jax.experimental import pallas as pl
from jax.experimental.pallas import tpu as pltpu
from jax.sharding import PartitionSpec as P


AUX_COEF = 0.01
OUT_SCALE = 2.0
ALL_AXES = ("ep", "etp")
BF16 = jnp.bfloat16
F32 = jnp.float32
MIB = 1 << 20
FF_STEP = 256

NEXT_PAIRS = (1, 0, 3, 2)
ENDS_PAIRS = (3, 2, 1, 0)


def mm(lhs, rhs):
    return jnp.dot(lhs, rhs, preferred_element_type=F32)


def mm_nt(lhs, rhs):
    return lax.dot_general(lhs, rhs, (((1,), (1,)), ((), ())), preferred_element_type=F32)


def mm_tn(lhs, rhs):
    return lax.dot_general(lhs, rhs, (((0,), (0,)), ((), ())), preferred_element_type=F32)


def params(vmem_mib, dims=1):
    return pltpu.CompilerParams(dimension_semantics=("arbitrary",) * dims, vmem_limit_bytes=vmem_mib * MIB)


def spread_kernel(n_etp, h_ref, dy_ref, h_all, dy_col, h_recv, dy_recv, z_send, x_send, y_send, c_send, own_sem):
    t = lax.axis_index("etp")
    o = lax.axis_index("ep")
    col_c = o + 1 - 2 * (o % 2)
    col_x = o + 2 - 4 * ((o // 2) % 2)
    col_y = o + 4 - 8 * (o // 4)
    col_d = col_x + 4 - 8 * (o // 4)
    order = [t, t + 1 - 2 * (t % 2), (t + 2) % 4, 3 - t]
    has_left, has_right = t > 0, t < n_etp - 1

    barrier = pltpu.get_barrier_semaphore()
    for col in (col_c, col_x, col_y):
        pl.semaphore_signal(barrier, inc=1, device_id={"ep": col}, device_id_type=pl.DeviceIdType.MESH)

    @pl.when(has_left)
    def _():
        pl.semaphore_signal(barrier, inc=1, device_id={"etp": t - 1}, device_id_type=pl.DeviceIdType.MESH)

    @pl.when(has_right)
    def _():
        pl.semaphore_signal(barrier, inc=1, device_id={"etp": t + 1}, device_id_type=pl.DeviceIdType.MESH)

    pl.semaphore_wait(barrier, 3 + (t + n_etp - 1) // n_etp + (2 * n_etp - 2 - t) // n_etp)

    keep = [pltpu.make_async_copy(h_ref, h_all.at[o * n_etp + t], own_sem.at[0]), pltpu.make_async_copy(dy_ref, dy_col.at[t], own_sem.at[1])]
    for copy in keep:
        copy.start()

    def h_copy(col, s, send_sem, to):
        slot = col * n_etp + s
        return pltpu.make_async_remote_copy(src_ref=h_all.at[slot], dst_ref=h_all.at[slot], send_sem=send_sem, recv_sem=h_recv.at[slot], device_id=to, device_id_type=pl.DeviceIdType.MESH)

    def own_copy(send_sem, to):
        slot = o * n_etp + t
        return pltpu.make_async_remote_copy(src_ref=h_ref, dst_ref=h_all.at[slot], send_sem=send_sem, recv_sem=h_recv.at[slot], device_id=to, device_id_type=pl.DeviceIdType.MESH)

    def dy_copy(s, send_sem, to, own=False):
        return pltpu.make_async_remote_copy(src_ref=dy_ref if own else dy_col.at[s], dst_ref=dy_col.at[s], send_sem=send_sem, recv_sem=dy_recv.at[s], device_id=to, device_id_type=pl.DeviceIdType.MESH)

    def h_arrived(col, s):
        h_copy(col, s, own_sem.at[0], {"ep": col_c}).wait_recv()

    def dy_arrived(s):
        dy_copy(s, own_sem.at[0], {"ep": col_c}).wait_recv()

    right, left = {"etp": t + 1}, {"etp": t - 1}
    to_x, to_y, to_c = {"ep": col_x}, {"ep": col_y}, {"ep": col_c}

    def z_copy(k, data, go):
        s, to, sem = (t - k, right, z_send.at[data, 0, k]) if go == 0 else (t + k, left, z_send.at[data, 1, k])
        if data == 0:
            return own_copy(sem, to) if k == 0 else h_copy(o, s, sem, to)
        return dy_copy(s, sem, to, own=k == 0)

    def z_goes(k, go):
        return has_right & (t >= k) if go == 0 else has_left & (t <= n_etp - 1 - k)

    def z_send_step(k, data):
        for go in (0, 1):
            pl.when(z_goes(k, go))(lambda: z_copy(k, data, go).start())

    def z_arrive(k, data):
        arrived = (lambda s: h_arrived(o, s)) if data == 0 else dy_arrived
        pl.when(t >= k)(lambda: arrived(t - k))
        pl.when(t <= n_etp - 1 - k)(lambda: arrived(t + k))

    def a_step(k):
        s = order[k]
        for sem, to in ((x_send.at[k], to_x), (y_send.at[k], to_y), (c_send.at[0, k], to_c)):
            (own_copy(sem, to) if k == 0 else h_copy(o, s, sem, to)).start()

    def b_step(k):
        s = order[k]
        h_arrived(col_x, s)
        if k % 2 == 0:
            h_copy(col_x, s, y_send.at[4 + k // 2], to_y).start()
        h_copy(col_x, s, c_send.at[1, k], to_c).start()
        h_arrived(col_y, s)
        if k % 2 == 1:
            h_copy(col_y, s, x_send.at[4 + k // 2], to_x).start()
        h_copy(col_y, s, c_send.at[2, k], to_c).start()

    def c_step(k):
        s = order[k]
        h_arrived(col_d, s)
        h_copy(col_d, s, c_send.at[3, k], to_c).start()

    z_send_step(0, 0)
    a_step(0)
    z_arrive(1, 0)
    z_send_step(1, 0)
    a_step(1)
    b_step(0)
    z_arrive(2, 0)
    z_send_step(2, 0)
    z_send_step(0, 1)
    a_step(2)
    b_step(1)
    z_arrive(3, 0)
    a_step(3)
    c_step(0)
    b_step(2)
    c_step(1)
    z_arrive(1, 1)
    z_send_step(1, 1)
    b_step(3)
    z_arrive(2, 1)
    z_send_step(2, 1)
    c_step(2)
    c_step(3)
    z_arrive(3, 1)

    for k in range(n_etp):
        for col in (col_x, col_y, col_d):
            h_arrived(col + 1 - 2 * (o % 2), order[k])
        h_arrived(col_c, order[k])
    for copy in keep:
        copy.wait()
    for k in range(n_etp - 1):
        for data in (0, 1):
            for go in (0, 1):
                pl.when(z_goes(k, go))(lambda: z_copy(k, data, go).wait_send())
    for i in range(6):
        h_copy(o, t, x_send.at[i], to_x).wait_send()
        h_copy(o, t, y_send.at[i], to_y).wait_send()
    for j in range(4):
        for k in range(n_etp):
            h_copy(o, t, c_send.at[j, k], to_c).wait_send()


def spread_all(h, dy, n_etp, n_ep):
    hbm = pl.BlockSpec(memory_space=pl.ANY)
    vmem = pl.BlockSpec(memory_space=pltpu.VMEM)
    dma = pltpu.SemaphoreType.DMA
    return pl.pallas_call(
        functools.partial(spread_kernel, n_etp),
        in_specs=[vmem, vmem],
        out_specs=[hbm, hbm],
        out_shape=[jax.ShapeDtypeStruct((n_ep * n_etp, *h.shape), h.dtype), jax.ShapeDtypeStruct((n_etp, *dy.shape), dy.dtype)],
        scratch_shapes=[dma((n_ep * n_etp,)), dma((n_etp,)), dma((2, 2, n_etp - 1)), dma((6,)), dma((6,)), dma((4, n_etp)), dma((2,))],
        compiler_params=pltpu.CompilerParams(collective_id=0, has_side_effects=True, vmem_limit_bytes=16 * MIB),
        cost_estimate=pl.CostEstimate(flops=10**11, bytes_accessed=2 * n_ep * n_etp * h.size, transcendentals=0),
        name="spread_all",
    )(h, dy)


PICK_STEP = 8


def pick_kernel(scaled, win, planes_ref, slots_ref, base_ref, src_ref, pos_ref, *rest):
    if scaled:
        gate_ref, out_ref, acc_ref = rest
    else:
        out_ref, acc_ref = rest
    grp = pl.program_id(0)
    blk = pl.program_id(1)

    @pl.when(blk == 0)
    def _():
        acc_ref[...] = jnp.zeros_like(acc_ref)

    parts = []
    for i in range(PICK_STEP):
        base = pl.multiple_of(base_ref[grp, blk * PICK_STEP + i], 8)
        pos_row = pos_ref[i, 0]
        want = base + lax.broadcasted_iota(jnp.int32, (win, pos_row.shape[1]), 0)
        hit = want == pos_row
        part = mm(hit.astype(F32).astype(BF16), src_ref[i, 0])
        if scaled:
            part = part * jnp.sum(jnp.where(hit, gate_ref[i, 0], 0.0), axis=1, keepdims=True)
        parts.append((base, part))
    for base, part in parts:
        acc_ref[pl.ds(base, win), :] += part

    @pl.when(blk == pl.num_programs(1) - 1)
    def _():
        out_ref[...] = acc_ref[: out_ref.shape[0], :].astype(out_ref.dtype)


def pick_rows(source, pos, gates, planes, slots, base, n_rows, win, n_src, n_etp):
    blk_rows = pos.shape[-1]
    d_model = source.shape[2]
    n_grp = planes.shape[0]
    src_map = lambda g, o, planes, slots, base: (o, slots[g], 0, 0)
    tab_map = lambda g, o, planes, slots, base: (o, planes[g], 0, 0)
    tab_spec = pl.BlockSpec((PICK_STEP, 1, 1, blk_rows), tab_map)
    tables = [table.reshape(n_src, n_etp, 1, blk_rows) for table in (pos, gates) if table is not None]
    flops = 2 * n_grp * n_src * win * blk_rows * d_model
    return pl.pallas_call(
        functools.partial(pick_kernel, gates is not None, win),
        grid_spec=pltpu.PrefetchScalarGridSpec(
            num_scalar_prefetch=3,
            grid=(n_grp, n_src // PICK_STEP),
            in_specs=[pl.BlockSpec((PICK_STEP, 1, blk_rows, d_model), src_map)] + [tab_spec] * len(tables),
            out_specs=pl.BlockSpec((n_rows, d_model), lambda g, o, planes, slots, base: (g, 0)),
            scratch_shapes=[pltpu.VMEM((n_rows + win, d_model), F32)],
        ),
        out_shape=jax.ShapeDtypeStruct((n_grp * n_rows, d_model), BF16),
        compiler_params=params(58, 2),
        cost_estimate=pl.CostEstimate(flops=flops, bytes_accessed=2 * source.size * 2, transcendentals=0),
        name="pick_rows",
    )(planes, slots, base, source.reshape(n_src, n_etp, *source.shape[1:]), *tables)


def whole(array):
    return pl.BlockSpec(array.shape, lambda i: (0, 0), pipeline_mode=pl.Buffered(1))


def sum_into(out_ref, base_ref, first, product):
    def step(i, _):
        cols = pl.ds(pl.multiple_of(i * FF_STEP, FF_STEP), FF_STEP)
        if not first:
            out_ref[:, cols] += product(cols)
        elif base_ref is not None:
            out_ref[:, cols] = base_ref[:, cols] + product(cols)
        else:
            out_ref[:, cols] = product(cols)
        return 0

    lax.fori_loop(0, out_ref.shape[1] // FF_STEP, step, 0, unroll=True)


def act_kernel(with_y, n_alias, x_ref, *refs):
    (w1, w3, *w2), refs = refs[: 2 + with_y], refs[2 + with_y + n_alias :]
    a_ref, b_ref, u_ref = refs[:3]

    def step(i, _):
        cols = pl.ds(pl.multiple_of(i * FF_STEP, FF_STEP), FF_STEP)
        act_a = mm(x_ref[...], w1[:, cols])
        act_b = mm(x_ref[...], w3[:, cols])
        a_ref[:, cols] = act_a
        b_ref[:, cols] = act_b
        u_ref[:, cols] = (act_a * jax.nn.sigmoid(act_a) * act_b).astype(BF16)
        return 0

    lax.fori_loop(0, w1.shape[1] // FF_STEP, step, 0, unroll=True)
    if with_y:
        sum_into(refs[3], None, True, lambda cols: mm(u_ref[...], w2[0][:, cols]))


def ffn_act(x, weights, tile, first, n_tiles, kept, total):
    d_model, d_ff = weights[0].shape
    with_y = len(weights) == 3
    rows = n_tiles * tile
    out_specs = [pl.BlockSpec((tile, d_ff), lambda i: (i + first, 0))] * 3
    out_shape = [jax.ShapeDtypeStruct((total, d_ff), dtype) for dtype in (F32, F32, BF16)]
    if with_y:
        out_specs.append(pl.BlockSpec((tile, d_model), lambda i: (i, 0)))
        out_shape.append(jax.ShapeDtypeStruct((rows, d_model), F32))
    n_in = 1 + len(weights)
    return pl.pallas_call(
        functools.partial(act_kernel, with_y, len(kept)),
        grid=(n_tiles,),
        in_specs=[pl.BlockSpec((tile, d_model), lambda i: (i + first, 0))] + [whole(w) for w in weights] + [pl.BlockSpec(memory_space=pl.ANY)] * len(kept),
        out_specs=out_specs,
        out_shape=out_shape,
        input_output_aliases={n_in + i: i for i in range(len(kept))},
        compiler_params=params(60),
        cost_estimate=pl.CostEstimate(flops=2 * len(weights) * rows * d_model * d_ff, bytes_accessed=6 * d_model * d_ff + 10 * rows * d_ff, transcendentals=rows * d_ff),
        name="ffn_act",
    )(x, *weights, *kept)


def down_kernel(u_ref, w2, y_in, y_ref):
    sum_into(y_ref, y_in, True, lambda cols: mm(u_ref[...], w2[:, cols]))


def ffn_down(u, w2, y_in, tile, first):
    d_ff, d_model = w2.shape
    return pl.pallas_call(
        down_kernel,
        grid=(1,),
        in_specs=[pl.BlockSpec((tile, d_ff), lambda i: (i + first, 0)), whole(w2), pl.BlockSpec((tile, d_model), lambda i: (i + first, 0))],
        out_specs=pl.BlockSpec((tile, d_model), lambda i: (i, 0)),
        out_shape=jax.ShapeDtypeStruct((tile, d_model), F32),
        compiler_params=params(48),
        cost_estimate=pl.CostEstimate(flops=2 * tile * d_model * d_ff, bytes_accessed=2 * d_model * d_ff + 8 * tile * d_model, transcendentals=0),
        name="ffn_down",
    )(u, w2, y_in)


def grad_kernel(with_dx, keeps, n_base, n_alias, c_ref, a_ref, b_ref, *refs):
    n_w = 3 if with_dx else 1
    (w2, *w13), base, refs = refs[:n_w], refs[n_w : n_w + n_base], list(refs[n_w + n_base + n_alias :])
    dx_ref = refs.pop(2 if keeps else 0) if with_dx else None
    da_ref, db_ref = refs

    def step(i, _):
        cols = pl.ds(pl.multiple_of(i * FF_STEP, FF_STEP), FF_STEP)
        d_inner = mm_nt(c_ref[...], w2[cols, :])
        act_a = a_ref[:, cols]
        sig_a = jax.nn.sigmoid(act_a)
        da_ref[:, cols] = (d_inner * b_ref[:, cols] * sig_a * (1.0 + act_a * (1.0 - sig_a))).astype(BF16)
        db_ref[:, cols] = (d_inner * (act_a * sig_a)).astype(BF16)
        return 0

    lax.fori_loop(0, w2.shape[0] // FF_STEP, step, 0, unroll=True)
    if with_dx:
        w1, w3 = w13
        sum_into(dx_ref, base[0] if base else None, True, lambda cols: mm_nt(da_ref[...], w1[cols, :]) + mm_nt(db_ref[...], w3[cols, :]))


def ffn_grad(c, act_a, act_b, weights, tile, first, first_act, n_tiles, kept, total=0, base=()):
    w2, *w13 = weights
    d_ff, d_model = w2.shape
    with_dx = bool(w13)
    rows = n_tiles * tile
    at = lambda width, start: pl.BlockSpec((tile, width), lambda i: (i + start, 0))
    out_specs = [at(d_ff, first)] * 2 if total else []
    out_shape = [jax.ShapeDtypeStruct((total, d_ff), BF16)] * 2 if total else []
    if with_dx:
        out_specs.append(at(d_model, 0))
        out_shape.append(jax.ShapeDtypeStruct((rows, d_model), F32))
    n_in = 3 + len(weights) + len(base)
    return pl.pallas_call(
        functools.partial(grad_kernel, with_dx, bool(total), len(base), len(kept)),
        grid=(n_tiles,),
        in_specs=[at(d_model, first), at(d_ff, first_act), at(d_ff, first_act)] + [whole(w) for w in weights] + [at(d_model, first)] * len(base) + [pl.BlockSpec(memory_space=pl.ANY)] * len(kept),
        out_specs=out_specs,
        out_shape=out_shape,
        scratch_shapes=[] if total else [pltpu.VMEM((tile, d_ff), BF16)] * 2,
        input_output_aliases={n_in + i: i for i in range(len(kept))},
        compiler_params=params(62),
        cost_estimate=pl.CostEstimate(flops=2 * len(weights) * rows * d_model * d_ff, bytes_accessed=6 * d_model * d_ff + 12 * rows * d_ff, transcendentals=rows * d_ff),
        name="ffn_grad",
    )(c, act_a, act_b, *weights, *base, *kept)


def bwd_kernel(n_sets, with_dx, with_y, n_alias, x_ref, c_ref, *refs):
    weights, refs = refs[: 3 * n_sets], list(refs[3 * n_sets + n_alias :])
    u_ref, da_ref, db_ref = refs[:3]
    dx_ref = refs.pop(3) if with_dx else None
    y_ref = refs.pop(3) if with_y else None
    tmp = refs[3:]
    for s in range(n_sets):
        w1, w3, w2 = weights[3 * s : 3 * s + 3]
        da, db, u = (da_ref, db_ref, u_ref) if s == 0 else (tmp[0], tmp[1], tmp[-1])
        with_u = s == 0 or with_y

        def step(i, _):
            cols = pl.ds(pl.multiple_of(i * FF_STEP, FF_STEP), FF_STEP)
            act_a = mm(x_ref[...], w1[:, cols])
            act_b = mm(x_ref[...], w3[:, cols])
            d_inner = mm_nt(c_ref[...], w2[cols, :])
            sig_a = jax.nn.sigmoid(act_a)
            silu_a = act_a * sig_a
            if with_u:
                u[:, cols] = (silu_a * act_b).astype(BF16)
            da[:, cols] = (d_inner * act_b * sig_a * (1.0 + act_a * (1.0 - sig_a))).astype(BF16)
            db[:, cols] = (d_inner * silu_a).astype(BF16)
            return 0

        lax.fori_loop(0, w1.shape[1] // FF_STEP, step, 0, unroll=True)
        if with_dx:
            sum_into(dx_ref, None, s == 0, lambda cols: mm_nt(da[...], w1[cols, :]) + mm_nt(db[...], w3[cols, :]))
        if with_y:
            sum_into(y_ref, None, s == 0, lambda cols: mm(u[...], w2[:, cols]))


def ffn_bwd(x, c, sets, tile, first, n_tiles, kept, with_dx=True, with_y=False):
    d_model, d_ff = sets[0].shape
    rows = n_tiles * tile
    n_sets = len(sets) // 3
    row_in = pl.BlockSpec((tile, d_model), lambda i: (i + first, 0))
    out_specs = [pl.BlockSpec((tile, d_ff), lambda i: (i + first, 0))] * 3
    out_shape = [jax.ShapeDtypeStruct((x.shape[0], d_ff), BF16)] * 3
    n_sums = int(with_dx) + int(with_y)
    out_specs += [pl.BlockSpec((tile, d_model), lambda i: (i, 0))] * n_sums
    out_shape += [jax.ShapeDtypeStruct((rows, d_model), F32)] * n_sums
    scratch = [pltpu.VMEM((tile, d_ff), BF16)] * (3 if with_y else 2) if n_sets > 1 else []
    n_in = 2 + len(sets)
    return pl.pallas_call(
        functools.partial(bwd_kernel, n_sets, with_dx, with_y, len(kept)),
        grid=(n_tiles,),
        in_specs=[row_in, row_in] + [whole(w) for w in sets] + [pl.BlockSpec(memory_space=pl.ANY)] * len(kept),
        out_specs=out_specs,
        out_shape=out_shape,
        scratch_shapes=scratch,
        input_output_aliases={n_in + i: i for i in range(len(kept))},
        compiler_params=params(60),
        cost_estimate=pl.CostEstimate(flops=(6 + 4 * with_dx + 2 * with_y) * rows * d_model * d_ff * n_sets, bytes_accessed=6 * d_model * d_ff * n_sets + 8 * rows * (d_model + d_ff), transcendentals=rows * d_ff * n_sets),
        name="ffn_bwd",
    )(x, c, *sets, *kept)


def pair_kernel(x_ref, c_ref, y_in, dx_in, w1, w3, w2, y_ref, dx_ref, u_ref, da_ref, db_ref):
    def step(i, _):
        cols = pl.ds(pl.multiple_of(i * FF_STEP, FF_STEP), FF_STEP)
        act_a = mm(x_ref[...], w1[:, cols])
        act_b = mm(x_ref[...], w3[:, cols])
        d_inner = mm_nt(c_ref[...], w2[cols, :])
        sig_a = jax.nn.sigmoid(act_a)
        silu_a = act_a * sig_a
        u_ref[:, cols] = (silu_a * act_b).astype(BF16)
        da_ref[:, cols] = (d_inner * act_b * sig_a * (1.0 + act_a * (1.0 - sig_a))).astype(BF16)
        db_ref[:, cols] = (d_inner * silu_a).astype(BF16)
        return 0

    lax.fori_loop(0, w1.shape[1] // FF_STEP, step, 0, unroll=True)
    sum_into(y_ref, y_in, True, lambda cols: mm(u_ref[...], w2[:, cols]))
    sum_into(dx_ref, dx_in, True, lambda cols: mm_nt(da_ref[...], w1[cols, :]) + mm_nt(db_ref[...], w3[cols, :]))


def ffn_pair(x, c, y_in, dx_in, weights, tile, first, n_tiles, first_dx):
    d_model, d_ff = weights[0].shape
    rows = n_tiles * tile
    at = lambda start: pl.BlockSpec((tile, d_model), lambda i: (i + start, 0))
    return pl.pallas_call(
        pair_kernel,
        grid=(n_tiles,),
        in_specs=[at(first), at(first), at(first), at(first_dx)] + [whole(w) for w in weights],
        out_specs=[at(0)] * 2,
        out_shape=[jax.ShapeDtypeStruct((rows, d_model), F32)] * 2,
        scratch_shapes=[pltpu.VMEM((tile, d_ff), BF16)] * 3,
        compiler_params=params(60),
        cost_estimate=pl.CostEstimate(flops=12 * rows * d_model * d_ff, bytes_accessed=6 * d_model * d_ff + 20 * rows * d_model, transcendentals=rows * d_ff),
        name="ffn_pair",
    )(x, c, y_in, dx_in, *weights)


def unset(*shapes):
    return pl.pallas_call(
        lambda *refs: None,
        out_specs=[pl.BlockSpec(memory_space=pl.ANY)] * len(shapes),
        out_shape=[jax.ShapeDtypeStruct(shape, BF16) for shape in shapes],
        name="unset",
    )()


def home_kernel(win, n_far, start_ref, near_ref, *refs):
    fars, (more_ref, out_ref, sum_ref) = refs[:n_far], refs[n_far:]
    row = 0
    for far in fars:
        rows = far.shape[0]
        sum_ref[row : row + rows, :] = (near_ref[row : row + rows, :] + far[...]).astype(BF16).astype(F32)
        row += rows
    sum_ref[row : row + more_ref.shape[0], :] = more_ref[...].astype(F32)
    row += more_ref.shape[0]
    sum_ref[row:, :] = jnp.zeros((sum_ref.shape[0] - row, sum_ref.shape[1]), F32)
    out_rows = out_ref.shape[1]
    to = lax.broadcasted_iota(jnp.int32, (out_rows, win), 0)
    frm = lax.broadcasted_iota(jnp.int32, (out_rows, win), 1)

    def block(o, _):
        start = start_ref[o]
        base = pl.multiple_of(start // 8 * 8, 8)
        rows = sum_ref[pl.ds(base, win), :].astype(BF16)
        move = (frm == to + (start - base)).astype(F32).astype(BF16)
        out_ref[o] = mm(move, rows).astype(BF16)
        return 0

    lax.fori_loop(0, out_ref.shape[0], block, 0)


def home_blocks(starts, near, fars, more, out_rows):
    n_out = starts.shape[0]
    d_model = near.shape[1]
    win = out_rows + 8
    vmem = pl.BlockSpec(memory_space=pltpu.VMEM)
    return pl.pallas_call(
        functools.partial(home_kernel, win, len(fars)),
        in_specs=[pl.BlockSpec(memory_space=pltpu.SMEM)] + [vmem] * (2 + len(fars)),
        out_specs=vmem,
        out_shape=jax.ShapeDtypeStruct((n_out, out_rows, d_model), BF16),
        scratch_shapes=[pltpu.VMEM((near.shape[0] + more.shape[0] + win, d_model), F32)],
        compiler_params=pltpu.CompilerParams(vmem_limit_bytes=40 * MIB),
        cost_estimate=pl.CostEstimate(flops=2 * n_out * out_rows * win * d_model, bytes_accessed=12 * near.size, transcendentals=0),
        name="home_blocks",
    )(starts, near, *fars, more)


def split3(value):
    high = lax.reduce_precision(value, 8, 7)
    rest = value - high
    mid = lax.reduce_precision(rest, 8, 7)
    return high.astype(BF16), mid.astype(BF16), (rest - mid).astype(BF16)


def solution(mesh):
    ep_size = mesh.shape["ep"]
    etp_size = mesh.shape["etp"]
    n_dev = ep_size * etp_size
    tok_spec = P(ALL_AXES, None)
    gate_spec = P("ep", None, "etp")
    down_spec = P("ep", "etp", None)

    def layer(hidden, w_router, expert_ids, d_out, w_gate, w_up, w_down):
        tok_rows, d_model = hidden.shape
        n_experts = w_router.shape[1]
        n_tokens = tok_rows * n_dev
        capacity = (5 * n_tokens + 2 * n_experts - 1) // (2 * n_experts)
        per_expert = 7 * tok_rows // (2 * n_experts)
        list_max = ep_size * per_expert
        main_rows = 23 * tok_rows // 8
        more_rows = list_max - main_rows
        tile = main_rows // 4
        win = per_expert + 8
        ep_i = lax.axis_index("ep")
        etp_i = lax.axis_index("etp")
        block_idx = ep_i * etp_size + etp_i
        w1, w3, w2 = w_gate[0], w_up[0], w_down[0]

        def swap(array, even, odd):
            pairs = [(t * ep_size + o, (odd if o % 2 else even)[t] * ep_size + o) for t in range(etp_size) for o in range(ep_size)]
            return lax.ppermute(array, ("etp", "ep"), pairs)

        ids_row = expert_ids.T.astype(BF16).reshape(1, 2 * tok_rows)
        ids_row = jnp.concatenate([ids_row, jnp.zeros((7, 2 * tok_rows), BF16)])
        h_all, dy_col = spread_all(jnp.concatenate([hidden, ids_row]), d_out, etp_size, ep_size)
        w1_b, w3_b, w2_b, h_all, dy_col = lax.optimization_barrier((w1, w3, w2, h_all, dy_col))
        w1p = swap(w1_b, NEXT_PAIRS, ENDS_PAIRS)
        w3p = swap(w3_b, NEXT_PAIRS, ENDS_PAIRS)
        w2p = swap(w2_b, NEXT_PAIRS, ENDS_PAIRS)
        dy_all = lax.all_gather(dy_col, "ep").reshape(n_dev, tok_rows, d_model)

        ids_all = h_all[:, tok_rows, :].astype(jnp.int32).reshape(n_dev, 2, tok_rows)
        id0, id1 = ids_all[:, 0], ids_all[:, 1]
        experts = jnp.arange(n_experts, dtype=jnp.int32)[None, :, None]
        count = jnp.sum(((id0[:, None, :] == experts) | (id1[:, None, :] == experts)).astype(F32), axis=2)
        before = jnp.cumsum(count, axis=0) - count
        kept = jnp.clip(capacity - before, 0, count).astype(jnp.int32)
        kept_lists = kept.reshape(ep_size, etp_size, n_experts)
        list_start = jnp.cumsum(kept_lists, axis=0) - kept_lists
        list_len = jnp.sum(kept_lists, axis=0)
        earlier = (jnp.arange(tok_rows)[:, None] < jnp.arange(tok_rows)[None, :]).astype(BF16)

        my_member = (id0 == ep_i) | (id1 == ep_i)
        my_rank = mm(my_member.astype(BF16), earlier).astype(jnp.int32)
        my_start = lax.dynamic_index_in_dim(list_start, ep_i, 2, keepdims=False)
        my_kept = lax.dynamic_index_in_dim(kept, ep_i, 1, keepdims=True)
        my_pos = jnp.where(my_member & (my_rank < my_kept), my_start.reshape(n_dev, 1) + my_rank, -1)
        odd = ep_i % 2
        far = jnp.where(odd == 1, etp_i ^ 1, etp_size - 1 - etp_i)
        planes = jnp.stack([far, etp_i, far ^ 2, etp_i ^ 2]).astype(jnp.int32)
        my_base = jnp.minimum(my_start, main_rows) // 8 * 8
        pick = functools.partial(pick_rows, win=win, n_src=ep_size, n_etp=etp_size)
        main_pos = jnp.where(my_pos < main_rows, my_pos, -1)
        main_base = my_base.T[planes]
        x_main = pick(h_all, main_pos, None, planes, planes, main_base, main_rows)

        route_w = jnp.concatenate(split3(w_router), axis=1)
        logit_parts = lax.dot_general(route_w, h_all, (((0,), (2,)), ((), ())), preferred_element_type=F32)[:, :, :tok_rows].reshape(-1, n_tokens)
        logits = logit_parts[:n_experts] + logit_parts[n_experts : 2 * n_experts] + logit_parts[2 * n_experts :]
        probs_all = jax.nn.softmax(logits, axis=0)
        expert_col = jnp.arange(n_experts, dtype=jnp.int32)[:, None]
        picked_all = jnp.where((id0.reshape(1, -1) == expert_col) | (id1.reshape(1, -1) == expert_col), probs_all, 0.0)
        my_gate = lax.dynamic_index_in_dim(picked_all, ep_i, 0, keepdims=False) / jnp.sum(picked_all, axis=0)
        mean_prob = jnp.sum(probs_all, axis=1) / n_tokens
        my_scale = OUT_SCALE * my_gate.reshape(n_dev, tok_rows)
        c_main = pick(dy_all, main_pos, my_scale, planes, planes, main_base, main_rows)

        n_rows = x_main.shape[0]
        *acts, y_base = ffn_act(x_main, (w1, w3, w2), tile, 0, 8, (), n_rows)
        act_a, act_b, inner = ffn_act(x_main, (w1, w3), tile, 8, 8, acts, n_rows)
        far_a, far_b, far_u = ffn_act(x_main, (w1p, w3p), tile, 0, 4, (), main_rows)
        *grads, dx_base = ffn_grad(c_main, act_a, act_b, (w2, w1, w3), tile, 0, 0, 4, (), n_rows)
        y_far, dx_far = [], []
        for i in range(2):
            y_part = ffn_down(far_u, w2p, y_base, 2 * tile, i)
            y_far.append(swap(y_part, ENDS_PAIRS, NEXT_PAIRS))
        for i in range(2):
            (dx_part,) = ffn_grad(c_main, far_a, far_b, (w2p, w1p, w3p), tile, 2 * i, 2 * i, 2, (), base=(dx_base,))
            dx_far.append(swap(dx_part, ENDS_PAIRS, NEXT_PAIRS))
        *grads, dx_base = ffn_grad(c_main, act_a, act_b, (w2, w1, w3), tile, 4, 4, 4, grads, n_rows)
        y_near, dx_near = ffn_pair(x_main, c_main, y_base, dx_base, (w1p, w3p, w2p), tile, 4, 4, 0)
        d_a, d_b = ffn_grad(c_main, act_a, act_b, (w2,), tile, 8, 8, 8, grads, n_rows)

        def more_work(*_):
            more_pos = jnp.where(my_pos >= main_rows, my_pos - main_rows, -1)
            more_base = jnp.clip(my_start.T - main_rows, 0, more_rows) // 8 * 8
            order = jnp.arange(etp_size, dtype=jnp.int32)
            x_more = pick(h_all, more_pos, None, order, order, more_base, more_rows)
            c_more = pick(dy_all, more_pos, my_scale, order, order, more_base, more_rows)
            *acts, dx_part, y_part = ffn_bwd(x_more, c_more, (w1, w3, w2), more_rows, 0, etp_size, (), with_y=True)
            y_more = lax.psum_scatter(y_part, "etp", scatter_dimension=0, tiled=True)
            dx_more = lax.psum_scatter(dx_part, "etp", scatter_dimension=0, tiled=True)
            return y_more.astype(BF16), dx_more.astype(BF16), x_more, c_more, *acts

        n_more = etp_size * more_rows
        none = jnp.zeros((more_rows, d_model), BF16)
        spare = none, none, *unset(*[(n_more, d_model)] * 2, *[(n_more, w1.shape[1])] * 3)
        any_more = jnp.max(list_len) > main_rows
        y_more, dx_more, x_more, c_more, *more_acts = lax.cond(any_more, more_work, lambda *spare: spare, *spare)

        def more_grads(*grads):
            inner_more, d_a_more, d_b_more = more_acts
            return grads[0] + mm_tn(x_more, d_a_more), grads[1] + mm_tn(x_more, d_b_more), grads[2] + mm_tn(inner_more, c_more)

        home_start = lax.dynamic_index_in_dim(my_start, etp_i, 1, keepdims=False)

        def send_home(near, fars, more):
            blocks = home_blocks(home_start, near, fars, more, per_expert)
            return lax.all_to_all(blocks, "ep", 0, 0, tiled=True).reshape(n_experts * per_expert, d_model)

        hot = [(expert_ids[:, k : k + 1] == experts[0].T).astype(F32) for k in range(2)]
        probs = lax.dynamic_slice_in_dim(probs_all, block_idx * tok_rows, tok_rows, 1).T
        picked = [jnp.sum(probs * hot[k], axis=1, keepdims=True) for k in range(2)]
        pick_sum = picked[0] + picked[1]
        gates = [picked[k] / pick_sum for k in range(2)]
        my_kept_row = lax.dynamic_index_in_dim(kept, block_idx, 0, keepdims=True).astype(F32)
        rank = mm_tn(earlier, (hot[0] + hot[1]).astype(BF16))
        slot_row = jnp.arange(n_experts * per_expert, dtype=jnp.int32)[None, :]
        chosen = []
        for k in range(2):
            rank_k = jnp.sum(rank * hot[k], axis=1, keepdims=True)
            kept_k = jnp.sum(my_kept_row * hot[k], axis=1, keepdims=True)
            slot_k = jnp.where(rank_k < kept_k, expert_ids[:, k : k + 1] * per_expert + rank_k.astype(jnp.int32), -1)
            chosen.append(slot_k == slot_row)

        dw1 = mm_tn(x_main, d_a)
        y_near, dw1, x_main = lax.optimization_barrier((y_near, dw1, x_main))
        y_back = send_home(y_near, y_far, y_more)
        dw3 = mm_tn(x_main, d_b)
        y_pair = [mm(chosen[k].astype(BF16), y_back) for k in range(2)]
        hidden_f = hidden.astype(F32)
        output = (hidden_f + OUT_SCALE * (gates[0] * y_pair[0] + gates[1] * y_pair[1])).astype(BF16)
        d_out_f = d_out.astype(F32)
        d_gates = [jnp.sum(OUT_SCALE * d_out_f * y_pair[k], axis=1, keepdims=True) for k in range(2)]

        route_frac = jnp.sum(count, axis=0) / (2 * n_tokens)
        aux_loss = AUX_COEF * n_experts * jnp.sum(route_frac * mean_prob)
        mix = gates[0] * d_gates[0] + gates[1] * d_gates[1]
        d_probs = (AUX_COEF * n_experts / n_tokens) * route_frac[None, :]
        for k in range(2):
            d_probs = d_probs + hot[k] * ((d_gates[k] - mix) / pick_sum)
        d_logits = probs * (d_probs - jnp.sum(probs * d_probs, axis=1, keepdims=True))
        d_router_part = lax.dot_general(d_logits, hidden_f, (((0,), (0,)), ((), ())), precision=lax.Precision.HIGHEST, preferred_element_type=F32)
        dx_near, dw3, d_router_part = lax.optimization_barrier((dx_near, dw3, d_router_part))
        d_router = jnp.sum(lax.all_gather(d_router_part, ALL_AXES), axis=0).T
        dx_back = send_home(dx_near, dx_far, dx_more)
        dw2 = mm_tn(inner, c_main)

        dw1, dw3, dw2 = lax.cond(any_more, more_grads, lambda *grads: grads, dw1, dw3, dw2)
        d_route = lax.dot_general(d_logits, w_router, (((1,), (1,)), ((), ())), precision=lax.Precision.HIGHEST, preferred_element_type=F32)
        dx_sum = mm((chosen[0] | chosen[1]).astype(BF16), dx_back)
        d_hidden = (d_out_f + dx_sum + d_route).astype(BF16)
        return output, d_hidden, d_router, aux_loss, dw1[None], dw3[None], dw2[None]

    return jax.shard_map(layer, mesh=mesh, in_specs=(tok_spec, P(), tok_spec, tok_spec, gate_spec, gate_spec, down_spec), out_specs=(tok_spec, tok_spec, P(), P(), gate_spec, gate_spec, down_spec), check_vma=False)
```

```python
import functools
import jax
import jax.numpy as jnp
from jax import lax
from jax.experimental import pallas as pl
from jax.experimental.pallas import tpu as pltpu
from jax.sharding import PartitionSpec as P


AUX_COEF = 0.01
OUT_SCALE = 2.0
ALL_AXES = ("ep", "etp")
BF16 = jnp.bfloat16
F32 = jnp.float32
MIB = 1 << 20
FF_STEP = 256

NEXT_PAIRS = (1, 0, 3, 2)
ENDS_PAIRS = (3, 2, 1, 0)


def mm(lhs, rhs):
    return jnp.dot(lhs, rhs, preferred_element_type=F32)


def mm_nt(lhs, rhs, precision=None):
    return lax.dot_general(lhs, rhs, (((1,), (1,)), ((), ())), precision=precision, preferred_element_type=F32)


def mm_tn(lhs, rhs, precision=None):
    return lax.dot_general(lhs, rhs, (((0,), (0,)), ((), ())), precision=precision, preferred_element_type=F32)


def params(vmem_mib):
    return pltpu.CompilerParams(dimension_semantics=("arbitrary",), vmem_limit_bytes=vmem_mib * MIB)


def cost(flops, bytes_accessed, transcendentals=0):
    return pl.CostEstimate(flops=flops, bytes_accessed=bytes_accessed, transcendentals=transcendentals)


def rows_at(rows, width, start=0):
    return pl.BlockSpec((rows, width), lambda i: (i + start, 0))


def by_columns(width, step):
    def at(i, carry):
        step(pl.ds(pl.multiple_of(i * FF_STEP, FF_STEP), FF_STEP))
        return carry

    lax.fori_loop(0, width // FF_STEP, at, 0, unroll=True)


def flip_col(col, bit):
    return col + bit * (1 - 2 * ((col // bit) % 2))


def one_hot(hit):
    return hit.astype(F32).astype(BF16)


def spread_kernel(n_etp, h_ref, dy_ref, h_all, dy_col, h_recv, dy_recv, z_send, x_send, y_send, c_send, own_sem):
    t = lax.axis_index("etp")
    o = lax.axis_index("ep")
    col_c, col_x, col_y = [flip_col(o, bit) for bit in (1, 2, 4)]
    col_d = flip_col(col_x, 4)
    order = [t, flip_col(t, 1), flip_col(t, 2), n_etp - 1 - t]
    has_left, has_right = t > 0, t < n_etp - 1

    barrier = pltpu.get_barrier_semaphore()
    for col in (col_c, col_x, col_y):
        pl.semaphore_signal(barrier, device_id={"ep": col}, device_id_type=pl.DeviceIdType.MESH)

    @pl.when(has_left)
    def _():
        pl.semaphore_signal(barrier, device_id={"etp": t - 1}, device_id_type=pl.DeviceIdType.MESH)

    @pl.when(has_right)
    def _():
        pl.semaphore_signal(barrier, device_id={"etp": t + 1}, device_id_type=pl.DeviceIdType.MESH)

    pl.semaphore_wait(barrier, 3 + (t + n_etp - 1) // n_etp + (2 * n_etp - 2 - t) // n_etp)

    keep = [pltpu.make_async_copy(h_ref, h_all.at[o * n_etp + t], own_sem.at[0]), pltpu.make_async_copy(dy_ref, dy_col.at[t], own_sem.at[1])]
    for copy in keep:
        copy.start()

    def h_copy(col, s, send_sem, to):
        slot = col * n_etp + s
        return pltpu.make_async_remote_copy(src_ref=h_all.at[slot], dst_ref=h_all.at[slot], send_sem=send_sem, recv_sem=h_recv.at[slot], device_id=to, device_id_type=pl.DeviceIdType.MESH)

    def own_copy(send_sem, to):
        slot = o * n_etp + t
        return pltpu.make_async_remote_copy(src_ref=h_ref, dst_ref=h_all.at[slot], send_sem=send_sem, recv_sem=h_recv.at[slot], device_id=to, device_id_type=pl.DeviceIdType.MESH)

    def dy_copy(s, send_sem, to, own=False):
        return pltpu.make_async_remote_copy(src_ref=dy_ref if own else dy_col.at[s], dst_ref=dy_col.at[s], send_sem=send_sem, recv_sem=dy_recv.at[s], device_id=to, device_id_type=pl.DeviceIdType.MESH)

    def h_arrived(col, s):
        h_copy(col, s, own_sem.at[0], {"ep": col_c}).wait_recv()

    def dy_arrived(s):
        dy_copy(s, own_sem.at[0], {"ep": col_c}).wait_recv()

    right, left = {"etp": t + 1}, {"etp": t - 1}
    to_x, to_y, to_c = {"ep": col_x}, {"ep": col_y}, {"ep": col_c}

    def z_copy(k, data, go):
        s, to, sem = (t - k, right, z_send.at[data, 0, k]) if go == 0 else (t + k, left, z_send.at[data, 1, k])
        if data == 0:
            return own_copy(sem, to) if k == 0 else h_copy(o, s, sem, to)
        return dy_copy(s, sem, to, own=k == 0)

    def z_goes(k, go):
        return has_right & (t >= k) if go == 0 else has_left & (t <= n_etp - 1 - k)

    def z_send_step(k, data):
        for go in (0, 1):
            pl.when(z_goes(k, go))(lambda: z_copy(k, data, go).start())

    def z_arrive(k, data):
        arrived = (lambda s: h_arrived(o, s)) if data == 0 else dy_arrived
        pl.when(t >= k)(lambda: arrived(t - k))
        pl.when(t <= n_etp - 1 - k)(lambda: arrived(t + k))

    def a_step(k):
        s = order[k]
        for sem, to in ((x_send.at[k], to_x), (y_send.at[k], to_y), (c_send.at[0, k], to_c)):
            (own_copy(sem, to) if k == 0 else h_copy(o, s, sem, to)).start()

    def b_step(k):
        s = order[k]
        h_arrived(col_x, s)
        if k % 2 == 0:
            h_copy(col_x, s, y_send.at[4 + k // 2], to_y).start()
        h_copy(col_x, s, c_send.at[1, k], to_c).start()
        h_arrived(col_y, s)
        if k % 2 == 1:
            h_copy(col_y, s, x_send.at[4 + k // 2], to_x).start()
        h_copy(col_y, s, c_send.at[2, k], to_c).start()

    def c_step(k):
        s = order[k]
        h_arrived(col_d, s)
        h_copy(col_d, s, c_send.at[3, k], to_c).start()

    steps = {
        "s": functools.partial(z_send_step, data=0),
        "S": functools.partial(z_send_step, data=1),
        "r": functools.partial(z_arrive, data=0),
        "R": functools.partial(z_arrive, data=1),
        "a": a_step,
        "b": b_step,
        "c": c_step,
    }
    plan = "s0a0r1s1a1b0r2s2S0a2b1r3a3c0b2c1R1S1b3R2S2c2c3R3"
    for kind, k in zip(plan[::2], plan[1::2]):
        steps[kind](int(k))

    for k in range(n_etp):
        for col in (col_x, col_y, col_d):
            h_arrived(flip_col(col, 1), order[k])
        h_arrived(col_c, order[k])
    for copy in keep:
        copy.wait()
    for k in range(n_etp - 1):
        for data in (0, 1):
            for go in (0, 1):
                pl.when(z_goes(k, go))(lambda: z_copy(k, data, go).wait_send())
    for i in range(6):
        h_copy(o, t, x_send.at[i], to_x).wait_send()
        h_copy(o, t, y_send.at[i], to_y).wait_send()
    for j in range(4):
        for k in range(n_etp):
            h_copy(o, t, c_send.at[j, k], to_c).wait_send()


def spread_all(h, dy, n_etp, n_ep):
    hbm = pl.BlockSpec(memory_space=pl.ANY)
    vmem = pl.BlockSpec(memory_space=pltpu.VMEM)
    dma = pltpu.SemaphoreType.DMA
    return pl.pallas_call(
        functools.partial(spread_kernel, n_etp),
        in_specs=[vmem, vmem],
        out_specs=[hbm, hbm],
        out_shape=[jax.ShapeDtypeStruct((n_ep * n_etp, *h.shape), h.dtype), jax.ShapeDtypeStruct((n_etp, *dy.shape), dy.dtype)],
        scratch_shapes=[dma((n_ep * n_etp,)), dma((n_etp,)), dma((2, 2, n_etp - 1)), dma((6,)), dma((6,)), dma((4, n_etp)), dma((2,))],
        compiler_params=pltpu.CompilerParams(collective_id=0, has_side_effects=True, vmem_limit_bytes=16 * MIB),
        cost_estimate=cost(10**11, 2 * n_ep * n_etp * h.size),
        name="spread_all",
    )(h, dy)


def pick_kernel(n_arrays, scaled, win, planes_ref, cols_ref, base_ref, *refs):
    sources, (pos_ref, *gate_ref, out_ref, acc_ref) = refs[:n_arrays], refs[n_arrays:]
    grp = pl.program_id(0)
    acc_ref[...] = jnp.zeros_like(acc_ref)
    for i in range(pos_ref.shape[0]):
        col = cols_ref[i]
        base = pl.multiple_of(base_ref[grp, col], 8)
        pos_row = pos_ref[col, 0]
        want = base + lax.broadcasted_iota(jnp.int32, (win, pos_row.shape[1]), 0)
        hit = want == pos_row
        block = sources[i][0] if n_arrays > 1 else sources[0][i, 0]
        part = mm(one_hot(hit), block)
        if scaled:
            part = part * jnp.sum(jnp.where(hit, gate_ref[0][col, 0], 0.0), axis=1, keepdims=True)
        acc_ref[pl.ds(base, win), :] += part
    out_ref[...] = acc_ref[: out_ref.shape[0], :].astype(out_ref.dtype)


def pick_rows(sources, cols, pos, gates, planes, base, n_rows, win, n_src, n_etp):
    blk_rows = pos.shape[-1]
    d_model = sources[0].shape[-1]
    n_grp = planes.shape[0]
    plane_map = lambda g, planes, cols, base: (0, planes[g], 0, 0)
    table_spec = pl.BlockSpec((n_src, 1, 1, blk_rows), plane_map)
    if len(sources) == 1:
        sources = [sources[0].reshape(n_src, n_etp, *sources[0].shape[1:])]
        source_spec = pl.BlockSpec((n_src, 1, blk_rows, d_model), plane_map)
    else:
        source_spec = pl.BlockSpec((1, blk_rows, d_model), lambda g, planes, cols, base: (planes[g], 0, 0))
    tables = [table.reshape(n_src, n_etp, 1, blk_rows) for table in (pos, gates) if table is not None]
    work = n_grp * n_src * blk_rows * d_model
    return pl.pallas_call(
        functools.partial(pick_kernel, len(sources), gates is not None, win),
        grid_spec=pltpu.PrefetchScalarGridSpec(
            num_scalar_prefetch=3,
            grid=(n_grp,),
            in_specs=[source_spec] * len(sources) + [table_spec] * len(tables),
            out_specs=pl.BlockSpec((n_rows, d_model), lambda g, planes, cols, base: (g, 0)),
            scratch_shapes=[pltpu.VMEM((n_rows + win, d_model), F32)],
        ),
        out_shape=jax.ShapeDtypeStruct((n_grp * n_rows, d_model), BF16),
        compiler_params=params(58),
        cost_estimate=cost(2 * win * work, 4 * work),
        name="pick_rows",
    )(planes, cols, base, *sources, *tables)


def whole(array):
    return pl.BlockSpec(array.shape, lambda i: (0, 0), pipeline_mode=pl.Buffered(1))


def sum_into(out_ref, base_ref, product):
    def step(cols):
        part = product(cols)
        out_ref[:, cols] = part if base_ref is None else base_ref[:, cols] + part

    by_columns(out_ref.shape[1], step)


def act_kernel(with_y, n_alias, x_ref, *refs):
    (w1, w3, *w2), refs = refs[: 2 + with_y], refs[2 + with_y + n_alias :]
    a_ref, b_ref, u_ref = refs[:3]

    def step(cols):
        act_a = mm(x_ref[...], w1[:, cols])
        act_b = mm(x_ref[...], w3[:, cols])
        a_ref[:, cols] = act_a
        b_ref[:, cols] = act_b
        u_ref[:, cols] = (act_a * jax.nn.sigmoid(act_a) * act_b).astype(BF16)

    by_columns(w1.shape[1], step)
    if with_y:
        sum_into(refs[3], None, lambda cols: mm(u_ref[...], w2[0][:, cols]))


def ffn_act(x, weights, tile, first, n_tiles, kept, total):
    d_model, d_ff = weights[0].shape
    with_y = len(weights) == 3
    rows = n_tiles * tile
    out_specs = [rows_at(tile, d_ff, first)] * 3
    out_shape = [jax.ShapeDtypeStruct((total, d_ff), dtype) for dtype in (F32, F32, BF16)]
    if with_y:
        out_specs.append(rows_at(tile, d_model))
        out_shape.append(jax.ShapeDtypeStruct((rows, d_model), F32))
    n_in = 1 + len(weights)
    return pl.pallas_call(
        functools.partial(act_kernel, with_y, len(kept)),
        grid=(n_tiles,),
        in_specs=[rows_at(tile, d_model, first)] + [whole(w) for w in weights] + [pl.BlockSpec(memory_space=pl.ANY)] * len(kept),
        out_specs=out_specs,
        out_shape=out_shape,
        input_output_aliases={n_in + i: i for i in range(len(kept))},
        compiler_params=params(60),
        cost_estimate=cost(2 * len(weights) * rows * d_model * d_ff, 6 * d_model * d_ff + 10 * rows * d_ff, rows * d_ff),
        name="ffn_act",
    )(x, *weights, *kept)


def down_kernel(u_ref, w2, y_in, y_ref):
    sum_into(y_ref, y_in, lambda cols: mm(u_ref[...], w2[:, cols]))


def ffn_down(u, w2, y_in, tile, first, n_tiles):
    d_ff, d_model = w2.shape
    rows = n_tiles * tile
    return pl.pallas_call(
        down_kernel,
        grid=(n_tiles,),
        in_specs=[rows_at(tile, d_ff, first), whole(w2), rows_at(tile, d_model, first)],
        out_specs=rows_at(tile, d_model),
        out_shape=jax.ShapeDtypeStruct((rows, d_model), F32),
        compiler_params=params(48),
        cost_estimate=cost(2 * rows * d_model * d_ff, 2 * d_model * d_ff + 8 * rows * d_model),
        name="ffn_down",
    )(u, w2, y_in)


def grad_kernel(with_dx, keeps, n_base, n_alias, c_ref, a_ref, b_ref, *refs):
    n_w = 3 if with_dx else 1
    (w2, *w13), base, refs = refs[:n_w], refs[n_w : n_w + n_base], list(refs[n_w + n_base + n_alias :])
    dx_ref = refs.pop(2 if keeps else 0) if with_dx else None
    da_ref, db_ref = refs

    def step(cols):
        d_inner = mm_nt(c_ref[...], w2[cols, :])
        act_a = a_ref[:, cols]
        sig_a = jax.nn.sigmoid(act_a)
        da_ref[:, cols] = (d_inner * b_ref[:, cols] * sig_a * (1.0 + act_a * (1.0 - sig_a))).astype(BF16)
        db_ref[:, cols] = (d_inner * (act_a * sig_a)).astype(BF16)

    by_columns(w2.shape[0], step)
    if with_dx:
        w1, w3 = w13
        sum_into(dx_ref, base[0] if base else None, lambda cols: mm_nt(da_ref[...], w1[cols, :]) + mm_nt(db_ref[...], w3[cols, :]))


def ffn_grad(c, act_a, act_b, weights, tile, first, first_act, n_tiles, kept, total=0, base=()):
    w2, *w13 = weights
    d_ff, d_model = w2.shape
    with_dx = bool(w13)
    rows = n_tiles * tile
    at = functools.partial(rows_at, tile)
    out_specs = [at(d_ff, first)] * 2 if total else []
    out_shape = [jax.ShapeDtypeStruct((total, d_ff), BF16)] * 2 if total else []
    if with_dx:
        out_specs.append(at(d_model))
        out_shape.append(jax.ShapeDtypeStruct((rows, d_model), F32))
    n_in = 3 + len(weights) + len(base)
    return pl.pallas_call(
        functools.partial(grad_kernel, with_dx, bool(total), len(base), len(kept)),
        grid=(n_tiles,),
        in_specs=[at(d_model, first), at(d_ff, first_act), at(d_ff, first_act)] + [whole(w) for w in weights] + [at(d_model, first)] * len(base) + [pl.BlockSpec(memory_space=pl.ANY)] * len(kept),
        out_specs=out_specs,
        out_shape=out_shape,
        scratch_shapes=[] if total else [pltpu.VMEM((tile, d_ff), BF16)] * 2,
        input_output_aliases={n_in + i: i for i in range(len(kept))},
        compiler_params=params(62),
        cost_estimate=cost(2 * len(weights) * rows * d_model * d_ff, 6 * d_model * d_ff + 12 * rows * d_ff, rows * d_ff),
        name="ffn_grad",
    )(c, act_a, act_b, *weights, *base, *kept)


def pair_kernel(x_ref, c_ref, y_in, dx_in, w1, w3, w2, y_ref, dx_ref, u_ref, da_ref, db_ref):
    def step(cols):
        act_a = mm(x_ref[...], w1[:, cols])
        act_b = mm(x_ref[...], w3[:, cols])
        d_inner = mm_nt(c_ref[...], w2[cols, :])
        sig_a = jax.nn.sigmoid(act_a)
        silu_a = act_a * sig_a
        u_ref[:, cols] = (silu_a * act_b).astype(BF16)
        da_ref[:, cols] = (d_inner * act_b * sig_a * (1.0 + act_a * (1.0 - sig_a))).astype(BF16)
        db_ref[:, cols] = (d_inner * silu_a).astype(BF16)

    by_columns(w1.shape[1], step)
    sum_into(y_ref, y_in, lambda cols: mm(u_ref[...], w2[:, cols]))
    sum_into(dx_ref, dx_in, lambda cols: mm_nt(da_ref[...], w1[cols, :]) + mm_nt(db_ref[...], w3[cols, :]))


def ffn_pair(x, c, y_in, dx_in, weights, tile, first, n_tiles, first_dx):
    d_model, d_ff = weights[0].shape
    rows = n_tiles * tile
    at = functools.partial(rows_at, tile, d_model)
    return pl.pallas_call(
        pair_kernel,
        grid=(n_tiles,),
        in_specs=[at(first), at(first), at(first), at(first_dx)] + [whole(w) for w in weights],
        out_specs=[at()] * 2,
        out_shape=[jax.ShapeDtypeStruct((rows, d_model), F32)] * 2,
        scratch_shapes=[pltpu.VMEM((tile, d_ff), BF16)] * 3,
        compiler_params=params(60),
        cost_estimate=cost(12 * rows * d_model * d_ff, 6 * d_model * d_ff + 20 * rows * d_model, rows * d_ff),
        name="ffn_pair",
    )(x, c, y_in, dx_in, *weights)


def unset(*shapes):
    return pl.pallas_call(
        lambda *refs: None,
        out_specs=[pl.BlockSpec(memory_space=pl.ANY)] * len(shapes),
        out_shape=[jax.ShapeDtypeStruct(shape, BF16) for shape in shapes],
        name="unset",
    )()


def home_kernel(win, n_far, start_ref, near_ref, *refs):
    fars, (more_ref, out_ref, sum_ref) = refs[:n_far], refs[n_far:]
    row = 0
    for far in fars:
        rows = far.shape[0]
        sum_ref[row : row + rows, :] = (near_ref[row : row + rows, :] + far[...]).astype(BF16).astype(F32)
        row += rows
    sum_ref[row : row + more_ref.shape[0], :] = more_ref[...].astype(F32)
    row += more_ref.shape[0]
    sum_ref[row:, :] = jnp.zeros((sum_ref.shape[0] - row, sum_ref.shape[1]), F32)
    out_rows = out_ref.shape[1]
    to = lax.broadcasted_iota(jnp.int32, (out_rows, win), 0)
    frm = lax.broadcasted_iota(jnp.int32, (out_rows, win), 1)

    def block(o, _):
        start = start_ref[o]
        base = pl.multiple_of(start // 8 * 8, 8)
        rows = sum_ref[pl.ds(base, win), :].astype(BF16)
        move = one_hot(frm == to + (start - base))
        out_ref[o] = mm(move, rows).astype(BF16)
        return 0

    lax.fori_loop(0, out_ref.shape[0], block, 0)


def home_blocks(starts, near, fars, more, out_rows):
    n_out = starts.shape[0]
    d_model = near.shape[1]
    win = out_rows + 8
    vmem = pl.BlockSpec(memory_space=pltpu.VMEM)
    return pl.pallas_call(
        functools.partial(home_kernel, win, len(fars)),
        in_specs=[pl.BlockSpec(memory_space=pltpu.SMEM)] + [vmem] * (2 + len(fars)),
        out_specs=vmem,
        out_shape=jax.ShapeDtypeStruct((n_out, out_rows, d_model), BF16),
        scratch_shapes=[pltpu.VMEM((near.shape[0] + more.shape[0] + win, d_model), F32)],
        compiler_params=pltpu.CompilerParams(vmem_limit_bytes=40 * MIB),
        cost_estimate=cost(2 * n_out * out_rows * win * d_model, 12 * near.size),
        name="home_blocks",
    )(starts, near, *fars, more)


def return_kernel(n_etp, start_ref, first_ref, near_ref, far_ref, more_ref, part_ref, slot_ref, rest_ref, out_ref, total_ref, sum_ref, send_ref, back_ref, z_part, col_part, col_sum, send_sem, back_sem, z_sem, col_sem):
    t = lax.axis_index("etp")
    o = lax.axis_index("ep")
    n_ep = send_ref.shape[0]

    def col_at(i):
        col = o
        for bit in (1, 2, 4):
            if i & bit:
                col = flip_col(col, bit)
        return col

    barrier = pltpu.get_barrier_semaphore()
    planes = [(t + k) % n_etp for k in range(1, n_etp)]
    for i in range(1, n_ep):
        pl.semaphore_signal(barrier, device_id={"ep": col_at(i)}, device_id_type=pl.DeviceIdType.MESH)
    for plane in planes:
        pl.semaphore_signal(barrier, device_id={"etp": plane}, device_id_type=pl.DeviceIdType.MESH)
    pl.semaphore_wait(barrier, n_ep - 1 + n_etp - 1)

    def to(src, dst, sem, got, peer):
        return pltpu.make_async_remote_copy(src_ref=src, dst_ref=dst, send_sem=sem, recv_sem=got, device_id=peer, device_id_type=pl.DeviceIdType.MESH)

    z_copies = [to(part_ref, z_part.at[t], z_sem.at[0, k], z_sem.at[1, t], {"etp": plane}) for k, plane in enumerate(planes)]
    for copy in z_copies:
        copy.start()

    rows = first_ref.shape[0]
    sum_ref[:rows, :] = first_ref[...]
    end = rows + far_ref.shape[0]
    sum_ref[rows:end, :] = (near_ref[...] + far_ref[...]).astype(BF16)
    sum_ref[end:, :] = more_ref[...]

    blk_rows = send_ref.shape[1]
    put = lax.broadcasted_iota(jnp.int32, (blk_rows, sum_ref.shape[0]), 0)
    frm = lax.broadcasted_iota(jnp.int32, (blk_rows, sum_ref.shape[0]), 1)
    order = [6, 7, 2, 4, 3, 5, 1, 0]
    copies = {i: to(send_ref.at[i], back_ref.at[o], send_sem.at[i], back_sem.at[o], {"ep": col_at(i)}) for i in order if i}
    for k, i in enumerate(order):
        move = one_hot(frm == put + start_ref[col_at(i)])
        block = mm(move, sum_ref[...]).astype(BF16)
        if i:
            send_ref[i] = block
        else:
            back_ref[o] = block
        if k:
            copies[order[k - 1]].start()

    z_part[t] = part_ref[...]
    for plane in planes:
        to(part_ref, z_part.at[plane], z_sem.at[0, 0], z_sem.at[1, plane], {"etp": plane}).wait_recv()
    total = z_part[0]
    for k in range(1, n_etp):
        total += z_part[k]
    col_sum[...] = total

    cols = lax.broadcasted_iota(jnp.int32, (slot_ref.shape[0], blk_rows), 1)
    acc = rest_ref[...]
    col_copies = {i: to(col_sum, col_part.at[o], col_sem.at[0, i], col_sem.at[1, o], {"ep": col_at(i)}) for i in range(1, n_ep)}
    for k, i in enumerate((0, 1, 2, 4, 3, 5, 6, 7)):
        col = col_at(i)
        if i:
            to(send_ref.at[i], back_ref.at[col], send_sem.at[i], back_sem.at[col], {"ep": col}).wait_recv()
        local = cols + col * blk_rows
        hit = (slot_ref[:, 0:1] == local) | (slot_ref[:, 1:2] == local)
        acc += mm(one_hot(hit), back_ref[col])
        if k == 1:
            for copy in col_copies.values():
                copy.start()
    out_ref[...] = acc.astype(out_ref.dtype)

    col_part[o] = col_sum[...]
    for i in range(1, n_ep):
        col = col_at(i)
        to(col_sum, col_part.at[col], col_sem.at[0, i], col_sem.at[1, col], {"ep": col}).wait_recv()
    total = col_part[0]
    for k in range(1, n_ep):
        total += col_part[k]
    total_ref[...] = total
    for copy in [*z_copies, *copies.values(), *col_copies.values()]:
        copy.wait_send()


def return_rows(starts, first, near, far, more, part, slots, rest, n_etp, n_ep, blk_rows):
    d_model = near.shape[1]
    half = far.shape[0]
    dma = pltpu.SemaphoreType.DMA
    vmem = lambda array: rows_at(*array.shape)
    blocks = pltpu.VMEM((n_ep, blk_rows, d_model), BF16)
    return pl.pallas_call(
        functools.partial(return_kernel, n_etp),
        grid=(1,),
        in_specs=[pl.BlockSpec(memory_space=pltpu.SMEM), vmem(first), rows_at(half, d_model, 1), vmem(far), vmem(more), vmem(part), vmem(slots), vmem(rest)],
        out_specs=[vmem(rest), vmem(part)],
        out_shape=[jax.ShapeDtypeStruct(rest.shape, BF16), jax.ShapeDtypeStruct(part.shape, F32)],
        scratch_shapes=[
            pltpu.VMEM((2 * half + more.shape[0], d_model), BF16),
            blocks,
            blocks,
            pltpu.VMEM((n_etp, *part.shape), F32),
            pltpu.VMEM((n_ep, *part.shape), F32),
            pltpu.VMEM(part.shape, F32),
            dma((n_ep,)),
            dma((n_ep,)),
            dma((2, n_etp)),
            dma((2, n_ep)),
        ],
        compiler_params=pltpu.CompilerParams(collective_id=1, has_side_effects=True, vmem_limit_bytes=56 * MIB),
        cost_estimate=cost(10**10, 12 * near.size),
        name="return_rows",
    )(starts, first, near, far, more, part, slots, rest)


def split3(value):
    high = lax.reduce_precision(value, 8, 7)
    rest = value - high
    mid = lax.reduce_precision(rest, 8, 7)
    return high.astype(BF16), mid.astype(BF16), (rest - mid).astype(BF16)


def solution(mesh):
    ep_size = mesh.shape["ep"]
    etp_size = mesh.shape["etp"]
    n_dev = ep_size * etp_size
    tok_spec = P(ALL_AXES, None)
    gate_spec = P("ep", None, "etp")
    down_spec = P("ep", "etp", None)

    def layer(hidden, w_router, expert_ids, d_out, w_gate, w_up, w_down):
        tok_rows, d_model = hidden.shape
        n_experts = w_router.shape[1]
        n_tokens = tok_rows * n_dev
        capacity = (5 * n_tokens + 2 * n_experts - 1) // (2 * n_experts)
        per_expert = 7 * tok_rows // (2 * n_experts)
        list_max = ep_size * per_expert
        main_rows = 23 * tok_rows // 8
        more_rows = list_max - main_rows
        tile = main_rows // 4
        win = per_expert + 8
        ep_i = lax.axis_index("ep")
        etp_i = lax.axis_index("etp")
        block_idx = ep_i * etp_size + etp_i
        w1, w3, w2 = w_gate[0], w_up[0], w_down[0]

        def swap(array, even, odd):
            pairs = [(t * ep_size + o, (odd if o % 2 else even)[t] * ep_size + o) for t in range(etp_size) for o in range(ep_size)]
            return lax.ppermute(array, ("etp", "ep"), pairs)

        ids_row = expert_ids.T.astype(BF16).reshape(1, 2 * tok_rows)
        ids_row = jnp.concatenate([ids_row, jnp.zeros((7, 2 * tok_rows), BF16)])
        h_all, dy_col = spread_all(jnp.concatenate([hidden, ids_row]), d_out, etp_size, ep_size)
        w1_b, w3_b, w2_b, h_all, dy_b = lax.optimization_barrier((w1, w3, w2, h_all, dy_col))
        w1p = swap(w1_b, NEXT_PAIRS, ENDS_PAIRS)
        w3p = swap(w3_b, NEXT_PAIRS, ENDS_PAIRS)
        w2p = swap(w2_b, NEXT_PAIRS, ENDS_PAIRS)

        def flip(array, bit):
            return lax.ppermute(array, "ep", [(o, o ^ bit) for o in range(ep_size)])

        half_z = etp_size // 2
        dy_c, dy_x, dy_y = [flip(dy_b, bit) for bit in (1, 2, 4)]
        dy_d = flip(dy_y[:half_z], 2), flip(dy_x[half_z:], 4)
        dy_cx, dy_cy = flip(dy_x, 1), flip(dy_y, 1)
        dy_d = jnp.concatenate(dy_d)
        dy_cd = flip(dy_d, 1)
        dy_all = [dy_b, dy_c, dy_x, dy_cx, dy_y, dy_cy, dy_d, dy_cd]
        dy_cols = (ep_i ^ jnp.arange(ep_size)).astype(jnp.int32)
        all_cols = jnp.arange(ep_size, dtype=jnp.int32)

        ids_all = h_all[:, tok_rows, :].astype(jnp.int32).reshape(n_dev, 2, tok_rows)
        id0, id1 = ids_all[:, 0], ids_all[:, 1]
        experts = jnp.arange(n_experts, dtype=jnp.int32)[None, :, None]
        count = jnp.sum(((id0[:, None, :] == experts) | (id1[:, None, :] == experts)).astype(F32), axis=2)
        before = jnp.cumsum(count, axis=0) - count
        kept = jnp.clip(capacity - before, 0, count).astype(jnp.int32)
        kept_lists = kept.reshape(ep_size, etp_size, n_experts)
        list_start = jnp.cumsum(kept_lists, axis=0) - kept_lists
        list_len = jnp.sum(kept_lists, axis=0)
        earlier = (jnp.arange(tok_rows)[:, None] < jnp.arange(tok_rows)[None, :]).astype(BF16)

        my_member = (id0 == ep_i) | (id1 == ep_i)
        my_rank = mm(my_member.astype(BF16), earlier).astype(jnp.int32)
        my_start = lax.dynamic_index_in_dim(list_start, ep_i, 2, keepdims=False)
        my_kept = lax.dynamic_index_in_dim(kept, ep_i, 1, keepdims=True)
        my_pos = jnp.where(my_member & (my_rank < my_kept), my_start.reshape(n_dev, 1) + my_rank, -1)
        odd = ep_i % 2
        far = jnp.where(odd == 1, etp_i ^ 1, etp_size - 1 - etp_i)
        planes = jnp.stack([far, etp_i, far ^ 2, etp_i ^ 2]).astype(jnp.int32)
        my_base = jnp.minimum(my_start, main_rows) // 8 * 8
        pick = functools.partial(pick_rows, win=win, n_src=ep_size, n_etp=etp_size)
        main_pos = jnp.where(my_pos < main_rows, my_pos, -1)
        main_base = my_base.T[planes]
        x_main = pick([h_all], all_cols, main_pos, None, planes, main_base, main_rows)

        route_w = jnp.concatenate(split3(w_router), axis=1)
        logit_parts = lax.dot_general(route_w, h_all, (((0,), (2,)), ((), ())), preferred_element_type=F32)[:, :, :tok_rows].reshape(-1, n_tokens)
        logits = logit_parts[:n_experts] + logit_parts[n_experts : 2 * n_experts] + logit_parts[2 * n_experts :]
        probs_all = jax.nn.softmax(logits, axis=0)
        expert_col = jnp.arange(n_experts, dtype=jnp.int32)[:, None]
        picked_all = jnp.where((id0.reshape(1, -1) == expert_col) | (id1.reshape(1, -1) == expert_col), probs_all, 0.0)
        my_gate = lax.dynamic_index_in_dim(picked_all, ep_i, 0, keepdims=False) / jnp.sum(picked_all, axis=0)
        mean_prob = jnp.sum(probs_all, axis=1) / n_tokens
        my_scale = OUT_SCALE * my_gate.reshape(n_dev, tok_rows)
        c_main = pick(dy_all, dy_cols, main_pos, my_scale, planes, main_base, main_rows)

        n_rows = x_main.shape[0]
        *acts, y_base = ffn_act(x_main, (w1, w3, w2), tile, 0, 8, (), n_rows)
        act_a, act_b, inner = ffn_act(x_main, (w1, w3), tile, 8, 8, acts, n_rows)
        far_a, far_b, far_u = ffn_act(x_main, (w1p, w3p), tile, 0, 4, (), main_rows)
        *grads, dx_base = ffn_grad(c_main, act_a, act_b, (w2, w1, w3), tile, 0, 0, 4, (), n_rows)
        y_far, dx_far = [], []
        for i, n_tiles in enumerate((1, 3)):
            y_part = ffn_down(far_u, w2p, y_base, tile, i, n_tiles)
            y_far.append(swap(y_part, ENDS_PAIRS, NEXT_PAIRS))
        for i in range(2):
            (dx_part,) = ffn_grad(c_main, far_a, far_b, (w2p, w1p, w3p), tile, 2 * i, 2 * i, 2, (), base=(dx_base,))
            dx_far.append(swap(dx_part, ENDS_PAIRS, NEXT_PAIRS))
        *grads, dx_base = ffn_grad(c_main, act_a, act_b, (w2, w1, w3), tile, 4, 4, 4, grads, n_rows)
        y_near, dx_near = ffn_pair(x_main, c_main, y_base, dx_base, (w1p, w3p, w2p), tile, 4, 4, 0)
        d_a, d_b = ffn_grad(c_main, act_a, act_b, (w2,), tile, 8, 8, 8, grads, n_rows)

        def add_planes(parts):
            total = parts[etp_i]
            for k in range(1, etp_size):
                shift = [(t, (t + k) % etp_size) for t in range(etp_size)]
                total += lax.ppermute(parts[(etp_i + k) % etp_size], "etp", shift)
            return total

        def more_work(*_):
            more_pos = jnp.where(my_pos >= main_rows, my_pos - main_rows, -1)
            more_base = jnp.clip(my_start.T - main_rows, 0, more_rows) // 8 * 8
            order = jnp.arange(etp_size, dtype=jnp.int32)
            x_more = pick([h_all], all_cols, more_pos, None, order, more_base, more_rows)
            c_more = pick(dy_all, dy_cols, more_pos, my_scale, order, more_base, more_rows)
            act_a, act_b, inner, y_part = ffn_act(x_more, (w1, w3, w2), more_rows, 0, etp_size, (), n_more)
            d_a, d_b, dx_part = ffn_grad(c_more, act_a, act_b, (w2, w1, w3), more_rows, 0, 0, etp_size, (), n_more)
            sums = [add_planes(part.reshape(etp_size, more_rows, d_model)).astype(BF16) for part in (y_part, dx_part)]
            return *sums, x_more, c_more, inner, d_a, d_b

        n_more = etp_size * more_rows
        none = jnp.zeros((more_rows, d_model), BF16)
        spare = none, none, *unset(*[(n_more, d_model)] * 2, *[(n_more, w1.shape[1])] * 3)
        any_more = jnp.max(list_len) > main_rows
        y_more, dx_more, x_more, c_more, *more_acts = lax.cond(any_more, more_work, lambda *spare: spare, *spare)

        def more_grads(*grads):
            inner_more, d_a_more, d_b_more = more_acts
            return grads[0] + mm_tn(x_more, d_a_more), grads[1] + mm_tn(x_more, d_b_more), grads[2] + mm_tn(inner_more, c_more)

        home_start = lax.dynamic_index_in_dim(my_start, etp_i, 1, keepdims=False)

        hot = [(expert_ids[:, k : k + 1] == experts[0].T).astype(F32) for k in range(2)]
        probs = lax.dynamic_slice_in_dim(probs_all, block_idx * tok_rows, tok_rows, 1).T
        picked = [jnp.sum(probs * hot[k], axis=1, keepdims=True) for k in range(2)]
        pick_sum = picked[0] + picked[1]
        gates = [picked[k] / pick_sum for k in range(2)]
        my_kept_row = lax.dynamic_index_in_dim(kept, block_idx, 0, keepdims=True).astype(F32)
        rank = mm_tn(earlier, (hot[0] + hot[1]).astype(BF16))
        slot_row = jnp.arange(n_experts * per_expert, dtype=jnp.int32)[None, :]
        slots, chosen = [], []
        for k in range(2):
            rank_k = jnp.sum(rank * hot[k], axis=1, keepdims=True)
            kept_k = jnp.sum(my_kept_row * hot[k], axis=1, keepdims=True)
            slot_k = jnp.where(rank_k < kept_k, expert_ids[:, k : k + 1] * per_expert + rank_k.astype(jnp.int32), -1)
            slots.append(slot_k)
            chosen.append(slot_k == slot_row)

        dw1 = mm_tn(x_main, d_a)
        y_near, dw1, x_main = lax.optimization_barrier((y_near, dw1, x_main))
        y_back = home_blocks(home_start, y_near, y_far, y_more, per_expert)
        y_back = lax.all_to_all(y_back, "ep", 0, 0, tiled=True).reshape(n_experts * per_expert, d_model)
        dw3 = mm_tn(x_main, d_b)
        dw2 = mm_tn(inner, c_main)
        dw1, dw3, dw2 = lax.cond(any_more, more_grads, lambda *grads: grads, dw1, dw3, dw2)
        y_pair = [mm(chosen[k].astype(BF16), y_back) for k in range(2)]
        hidden_f = hidden.astype(F32)
        output = (hidden_f + OUT_SCALE * (gates[0] * y_pair[0] + gates[1] * y_pair[1])).astype(BF16)
        d_out_f = d_out.astype(F32)
        d_gates = [jnp.sum(OUT_SCALE * d_out_f * y_pair[k], axis=1, keepdims=True) for k in range(2)]

        route_frac = jnp.sum(count, axis=0) / (2 * n_tokens)
        aux_loss = AUX_COEF * n_experts * jnp.sum(route_frac * mean_prob)
        mix = gates[0] * d_gates[0] + gates[1] * d_gates[1]
        d_probs = (AUX_COEF * n_experts / n_tokens) * route_frac[None, :]
        for k in range(2):
            d_probs = d_probs + hot[k] * ((d_gates[k] - mix) / pick_sum)
        d_logits = probs * (d_probs - jnp.sum(probs * d_probs, axis=1, keepdims=True))
        d_router_part = mm_tn(d_logits, hidden_f, lax.Precision.HIGHEST)
        d_route = mm_nt(d_logits, w_router, lax.Precision.HIGHEST)
        rest = d_out_f + d_route
        rest, first_far = lax.optimization_barrier((rest, dx_far[0]))
        first_dx = (dx_near[: main_rows // 2] + first_far).astype(BF16)
        dx_near, dw1, dw3, dw2, rest, first_dx, output = lax.optimization_barrier((dx_near, dw1, dw3, dw2, rest, first_dx, output))
        d_hidden, d_router = return_rows(home_start, first_dx, dx_near, dx_far[1], dx_more, d_router_part, jnp.concatenate(slots, axis=1), rest, etp_size, ep_size, per_expert)
        d_router = d_router.T
        return output, d_hidden, d_router, aux_loss, dw1[None], dw3[None], dw2[None]

    return jax.shard_map(layer, mesh=mesh, in_specs=(tok_spec, P(), tok_spec, tok_spec, gate_spec, gate_spec, down_spec), out_specs=(tok_spec, tok_spec, P(), P(), gate_spec, gate_spec, down_spec), check_vma=False)
```

```python
import functools
import jax
import jax.numpy as jnp
from jax import lax
from jax.experimental import pallas as pl
from jax.experimental.pallas import tpu as pltpu
from jax.sharding import PartitionSpec as P


AUX_COEF = 0.01
OUT_SCALE = 2.0
ALL_AXES = ("ep", "etp")
BF16 = jnp.bfloat16
F32 = jnp.float32
MIB = 1 << 20
FF_STEP = 256

NEXT_PAIRS = (1, 0, 3, 2)
ENDS_PAIRS = (3, 2, 1, 0)


def mm(lhs, rhs):
    return jnp.dot(lhs, rhs, preferred_element_type=F32)


def mm_nt(lhs, rhs, precision=None):
    return lax.dot_general(lhs, rhs, (((1,), (1,)), ((), ())), precision=precision, preferred_element_type=F32)


def mm_tn(lhs, rhs, precision=None):
    return lax.dot_general(lhs, rhs, (((0,), (0,)), ((), ())), precision=precision, preferred_element_type=F32)


def params(vmem_mib):
    return pltpu.CompilerParams(dimension_semantics=("arbitrary",), vmem_limit_bytes=vmem_mib * MIB)


def cost(flops, bytes_accessed, transcendentals=0):
    return pl.CostEstimate(flops=flops, bytes_accessed=bytes_accessed, transcendentals=transcendentals)


def rows_at(rows, width, start=0):
    return pl.BlockSpec((rows, width), lambda i: (i + start, 0))


def by_columns(width, step):
    def at(i, carry):
        step(pl.ds(pl.multiple_of(i * FF_STEP, FF_STEP), FF_STEP))
        return carry

    lax.fori_loop(0, width // FF_STEP, at, 0, unroll=True)


def flip_col(col, bit):
    return col + bit * (1 - 2 * ((col // bit) % 2))


def one_hot(hit):
    return hit.astype(F32).astype(BF16)


def spread_kernel(n_etp, h_ref, dy_ref, h_all, dy_col, h_recv, dy_recv, z_send, x_send, y_send, c_send, own_sem):
    t = lax.axis_index("etp")
    o = lax.axis_index("ep")
    col_c, col_x, col_y = [flip_col(o, bit) for bit in (1, 2, 4)]
    col_d = flip_col(col_x, 4)
    order = [t, flip_col(t, 1), flip_col(t, 2), n_etp - 1 - t]
    has_left, has_right = t > 0, t < n_etp - 1

    barrier = pltpu.get_barrier_semaphore()
    for col in (col_c, col_x, col_y):
        pl.semaphore_signal(barrier, device_id={"ep": col}, device_id_type=pl.DeviceIdType.MESH)

    @pl.when(has_left)
    def _():
        pl.semaphore_signal(barrier, device_id={"etp": t - 1}, device_id_type=pl.DeviceIdType.MESH)

    @pl.when(has_right)
    def _():
        pl.semaphore_signal(barrier, device_id={"etp": t + 1}, device_id_type=pl.DeviceIdType.MESH)

    pl.semaphore_wait(barrier, 3 + (t + n_etp - 1) // n_etp + (2 * n_etp - 2 - t) // n_etp)

    keep = [pltpu.make_async_copy(h_ref, h_all.at[o * n_etp + t], own_sem.at[0]), pltpu.make_async_copy(dy_ref, dy_col.at[t], own_sem.at[1])]
    for copy in keep:
        copy.start()

    def h_copy(col, s, send_sem, to):
        slot = col * n_etp + s
        return pltpu.make_async_remote_copy(src_ref=h_all.at[slot], dst_ref=h_all.at[slot], send_sem=send_sem, recv_sem=h_recv.at[slot], device_id=to, device_id_type=pl.DeviceIdType.MESH)

    def own_copy(send_sem, to):
        slot = o * n_etp + t
        return pltpu.make_async_remote_copy(src_ref=h_ref, dst_ref=h_all.at[slot], send_sem=send_sem, recv_sem=h_recv.at[slot], device_id=to, device_id_type=pl.DeviceIdType.MESH)

    def dy_copy(s, send_sem, to, own=False):
        return pltpu.make_async_remote_copy(src_ref=dy_ref if own else dy_col.at[s], dst_ref=dy_col.at[s], send_sem=send_sem, recv_sem=dy_recv.at[s], device_id=to, device_id_type=pl.DeviceIdType.MESH)

    def h_arrived(col, s):
        h_copy(col, s, own_sem.at[0], {"ep": col_c}).wait_recv()

    def dy_arrived(s):
        dy_copy(s, own_sem.at[0], {"ep": col_c}).wait_recv()

    right, left = {"etp": t + 1}, {"etp": t - 1}
    to_x, to_y, to_c = {"ep": col_x}, {"ep": col_y}, {"ep": col_c}

    def z_copy(k, data, go):
        s, to, sem = (t - k, right, z_send.at[data, 0, k]) if go == 0 else (t + k, left, z_send.at[data, 1, k])
        if data == 0:
            return own_copy(sem, to) if k == 0 else h_copy(o, s, sem, to)
        return dy_copy(s, sem, to, own=k == 0)

    def z_goes(k, go):
        return has_right & (t >= k) if go == 0 else has_left & (t <= n_etp - 1 - k)

    def z_send_step(k, data):
        for go in (0, 1):
            pl.when(z_goes(k, go))(lambda: z_copy(k, data, go).start())

    def z_arrive(k, data):
        arrived = (lambda s: h_arrived(o, s)) if data == 0 else dy_arrived
        pl.when(t >= k)(lambda: arrived(t - k))
        pl.when(t <= n_etp - 1 - k)(lambda: arrived(t + k))

    def a_step(k):
        s = order[k]
        for sem, to in ((x_send.at[k], to_x), (y_send.at[k], to_y), (c_send.at[0, k], to_c)):
            (own_copy(sem, to) if k == 0 else h_copy(o, s, sem, to)).start()

    def b_step(k):
        s = order[k]
        h_arrived(col_x, s)
        if k % 2 == 0:
            h_copy(col_x, s, y_send.at[4 + k // 2], to_y).start()
        h_copy(col_x, s, c_send.at[1, k], to_c).start()
        h_arrived(col_y, s)
        if k % 2 == 1:
            h_copy(col_y, s, x_send.at[4 + k // 2], to_x).start()
        h_copy(col_y, s, c_send.at[2, k], to_c).start()

    def c_step(k):
        s = order[k]
        h_arrived(col_d, s)
        h_copy(col_d, s, c_send.at[3, k], to_c).start()

    steps = {
        "s": functools.partial(z_send_step, data=0),
        "S": functools.partial(z_send_step, data=1),
        "r": functools.partial(z_arrive, data=0),
        "R": functools.partial(z_arrive, data=1),
        "a": a_step,
        "b": b_step,
        "c": c_step,
    }
    plan = "s0a0r1s1a1b0r2s2S0a2b1r3a3c0b2c1R1S1b3R2S2c2c3R3"
    for kind, k in zip(plan[::2], plan[1::2]):
        steps[kind](int(k))

    for k in range(n_etp):
        for col in (col_x, col_y, col_d):
            h_arrived(flip_col(col, 1), order[k])
        h_arrived(col_c, order[k])
    for copy in keep:
        copy.wait()
    for k in range(n_etp - 1):
        for data in (0, 1):
            for go in (0, 1):
                pl.when(z_goes(k, go))(lambda: z_copy(k, data, go).wait_send())
    for i in range(6):
        h_copy(o, t, x_send.at[i], to_x).wait_send()
        h_copy(o, t, y_send.at[i], to_y).wait_send()
    for j in range(4):
        for k in range(n_etp):
            h_copy(o, t, c_send.at[j, k], to_c).wait_send()


def spread_all(h, dy, n_etp, n_ep):
    hbm = pl.BlockSpec(memory_space=pl.ANY)
    vmem = pl.BlockSpec(memory_space=pltpu.VMEM)
    dma = pltpu.SemaphoreType.DMA
    return pl.pallas_call(
        functools.partial(spread_kernel, n_etp),
        in_specs=[vmem, vmem],
        out_specs=[hbm, hbm],
        out_shape=[jax.ShapeDtypeStruct((n_ep * n_etp, *h.shape), h.dtype), jax.ShapeDtypeStruct((n_etp, *dy.shape), dy.dtype)],
        scratch_shapes=[dma((n_ep * n_etp,)), dma((n_etp,)), dma((2, 2, n_etp - 1)), dma((6,)), dma((6,)), dma((4, n_etp)), dma((2,))],
        compiler_params=pltpu.CompilerParams(collective_id=0, has_side_effects=True, vmem_limit_bytes=16 * MIB),
        cost_estimate=cost(10**11, 2 * n_ep * n_etp * h.size),
        name="spread_all",
    )(h, dy)


def pick_kernel(n_arrays, scaled, win, planes_ref, cols_ref, base_ref, *refs):
    sources, (pos_ref, *gate_ref, out_ref, acc_ref) = refs[:n_arrays], refs[n_arrays:]
    grp = pl.program_id(0)
    acc_ref[...] = jnp.zeros_like(acc_ref)
    for i in range(pos_ref.shape[0]):
        col = cols_ref[i]
        base = pl.multiple_of(base_ref[grp, col], 8)
        pos_row = pos_ref[col, 0]
        want = base + lax.broadcasted_iota(jnp.int32, (win, pos_row.shape[1]), 0)
        hit = want == pos_row
        block = sources[i][0] if n_arrays > 1 else sources[0][i, 0]
        part = mm(one_hot(hit), block)
        if scaled:
            part = part * jnp.sum(jnp.where(hit, gate_ref[0][col, 0], 0.0), axis=1, keepdims=True)
        acc_ref[pl.ds(base, win), :] += part
    out_ref[...] = acc_ref[: out_ref.shape[0], :].astype(out_ref.dtype)


def pick_rows(sources, cols, pos, gates, planes, base, n_rows, win, n_src, n_etp):
    blk_rows = pos.shape[-1]
    d_model = sources[0].shape[-1]
    n_grp = planes.shape[0]
    plane_map = lambda g, planes, cols, base: (0, planes[g], 0, 0)
    table_spec = pl.BlockSpec((n_src, 1, 1, blk_rows), plane_map)
    if len(sources) == 1:
        sources = [sources[0].reshape(n_src, n_etp, *sources[0].shape[1:])]
        source_spec = pl.BlockSpec((n_src, 1, blk_rows, d_model), plane_map)
    else:
        source_spec = pl.BlockSpec((1, blk_rows, d_model), lambda g, planes, cols, base: (planes[g], 0, 0))
    tables = [table.reshape(n_src, n_etp, 1, blk_rows) for table in (pos, gates) if table is not None]
    work = n_grp * n_src * blk_rows * d_model
    return pl.pallas_call(
        functools.partial(pick_kernel, len(sources), gates is not None, win),
        grid_spec=pltpu.PrefetchScalarGridSpec(
            num_scalar_prefetch=3,
            grid=(n_grp,),
            in_specs=[source_spec] * len(sources) + [table_spec] * len(tables),
            out_specs=pl.BlockSpec((n_rows, d_model), lambda g, planes, cols, base: (g, 0)),
            scratch_shapes=[pltpu.VMEM((n_rows + win, d_model), F32)],
        ),
        out_shape=jax.ShapeDtypeStruct((n_grp * n_rows, d_model), BF16),
        compiler_params=params(58),
        cost_estimate=cost(2 * win * work, 4 * work),
        name="pick_rows",
    )(planes, cols, base, *sources, *tables)


def whole(array):
    return pl.BlockSpec(array.shape, lambda i: (0, 0), pipeline_mode=pl.Buffered(1))


def sum_into(out_ref, base_ref, product):
    def step(cols):
        part = product(cols)
        out_ref[:, cols] = part if base_ref is None else base_ref[:, cols] + part

    by_columns(out_ref.shape[1], step)


def act_kernel(with_y, n_alias, x_ref, *refs):
    (w1, w3, *w2), refs = refs[: 2 + with_y], refs[2 + with_y + n_alias :]
    a_ref, b_ref, u_ref = refs[:3]

    def step(cols):
        act_a = mm(x_ref[...], w1[:, cols])
        act_b = mm(x_ref[...], w3[:, cols])
        a_ref[:, cols] = act_a
        b_ref[:, cols] = act_b
        u_ref[:, cols] = (act_a * jax.nn.sigmoid(act_a) * act_b).astype(BF16)

    by_columns(w1.shape[1], step)
    if with_y:
        sum_into(refs[3], None, lambda cols: mm(u_ref[...], w2[0][:, cols]))


def ffn_act(x, weights, tile, first, n_tiles, kept, total):
    d_model, d_ff = weights[0].shape
    with_y = len(weights) == 3
    rows = n_tiles * tile
    out_specs = [rows_at(tile, d_ff, first)] * 3
    out_shape = [jax.ShapeDtypeStruct((total, d_ff), dtype) for dtype in (F32, F32, BF16)]
    if with_y:
        out_specs.append(rows_at(tile, d_model))
        out_shape.append(jax.ShapeDtypeStruct((rows, d_model), F32))
    n_in = 1 + len(weights)
    return pl.pallas_call(
        functools.partial(act_kernel, with_y, len(kept)),
        grid=(n_tiles,),
        in_specs=[rows_at(tile, d_model, first)] + [whole(w) for w in weights] + [pl.BlockSpec(memory_space=pl.ANY)] * len(kept),
        out_specs=out_specs,
        out_shape=out_shape,
        input_output_aliases={n_in + i: i for i in range(len(kept))},
        compiler_params=params(60),
        cost_estimate=cost(2 * len(weights) * rows * d_model * d_ff, 6 * d_model * d_ff + 10 * rows * d_ff, rows * d_ff),
        name="ffn_act",
    )(x, *weights, *kept)


def down_kernel(u_ref, w2, y_in, y_ref):
    sum_into(y_ref, y_in, lambda cols: mm(u_ref[...], w2[:, cols]))


def ffn_down(u, w2, y_in, tile, first, n_tiles):
    d_ff, d_model = w2.shape
    rows = n_tiles * tile
    return pl.pallas_call(
        down_kernel,
        grid=(n_tiles,),
        in_specs=[rows_at(tile, d_ff, first), whole(w2), rows_at(tile, d_model, first)],
        out_specs=rows_at(tile, d_model),
        out_shape=jax.ShapeDtypeStruct((rows, d_model), F32),
        compiler_params=params(48),
        cost_estimate=cost(2 * rows * d_model * d_ff, 2 * d_model * d_ff + 8 * rows * d_model),
        name="ffn_down",
    )(u, w2, y_in)


def grad_kernel(with_dx, keeps, n_base, n_alias, c_ref, a_ref, b_ref, *refs):
    n_w = 3 if with_dx else 1
    (w2, *w13), base, refs = refs[:n_w], refs[n_w : n_w + n_base], list(refs[n_w + n_base + n_alias :])
    dx_ref = refs.pop(2 if keeps else 0) if with_dx else None
    da_ref, db_ref = refs

    def step(cols):
        d_inner = mm_nt(c_ref[...], w2[cols, :])
        act_a = a_ref[:, cols]
        sig_a = jax.nn.sigmoid(act_a)
        da_ref[:, cols] = (d_inner * b_ref[:, cols] * sig_a * (1.0 + act_a * (1.0 - sig_a))).astype(BF16)
        db_ref[:, cols] = (d_inner * (act_a * sig_a)).astype(BF16)

    by_columns(w2.shape[0], step)
    if with_dx:
        w1, w3 = w13
        sum_into(dx_ref, base[0] if base else None, lambda cols: mm_nt(da_ref[...], w1[cols, :]) + mm_nt(db_ref[...], w3[cols, :]))


def ffn_grad(c, act_a, act_b, weights, tile, first, first_act, n_tiles, kept, total=0, base=(), dx_rows=0, first_dx=0):
    w2, *w13 = weights
    d_ff, d_model = w2.shape
    with_dx = bool(w13)
    rows = n_tiles * tile
    at = functools.partial(rows_at, tile)
    out_specs = [at(d_ff, first)] * 2 if total else []
    out_shape = [jax.ShapeDtypeStruct((total, d_ff), BF16)] * 2 if total else []
    if with_dx:
        out_specs.append(at(d_model, first_dx))
        out_shape.append(jax.ShapeDtypeStruct((dx_rows or rows, d_model), F32))
    n_in = 3 + len(weights) + len(base)
    return pl.pallas_call(
        functools.partial(grad_kernel, with_dx, bool(total), len(base), len(kept)),
        grid=(n_tiles,),
        in_specs=[at(d_model, first), at(d_ff, first_act), at(d_ff, first_act)] + [whole(w) for w in weights] + [at(d_model, first)] * len(base) + [pl.BlockSpec(memory_space=pl.ANY)] * len(kept),
        out_specs=out_specs,
        out_shape=out_shape,
        scratch_shapes=[] if total else [pltpu.VMEM((tile, d_ff), BF16)] * 2,
        input_output_aliases={n_in + i: i for i in range(len(kept))},
        compiler_params=params(62),
        cost_estimate=cost(2 * len(weights) * rows * d_model * d_ff, 6 * d_model * d_ff + 12 * rows * d_ff, rows * d_ff),
        name="ffn_grad",
    )(c, act_a, act_b, *weights, *base, *kept)


def pair_kernel(x_ref, c_ref, y_in, dx_in, w1, w3, w2, y_ref, dx_ref, u_ref, da_ref, db_ref):
    def step(cols):
        act_a = mm(x_ref[...], w1[:, cols])
        act_b = mm(x_ref[...], w3[:, cols])
        d_inner = mm_nt(c_ref[...], w2[cols, :])
        sig_a = jax.nn.sigmoid(act_a)
        silu_a = act_a * sig_a
        u_ref[:, cols] = (silu_a * act_b).astype(BF16)
        da_ref[:, cols] = (d_inner * act_b * sig_a * (1.0 + act_a * (1.0 - sig_a))).astype(BF16)
        db_ref[:, cols] = (d_inner * silu_a).astype(BF16)

    by_columns(w1.shape[1], step)
    sum_into(y_ref, y_in, lambda cols: mm(u_ref[...], w2[:, cols]))
    sum_into(dx_ref, dx_in, lambda cols: mm_nt(da_ref[...], w1[cols, :]) + mm_nt(db_ref[...], w3[cols, :]))


def ffn_pair(x, c, y_in, dx_in, weights, tile, first, n_tiles, first_dx):
    d_model, d_ff = weights[0].shape
    rows = n_tiles * tile
    at = functools.partial(rows_at, tile, d_model)
    return pl.pallas_call(
        pair_kernel,
        grid=(n_tiles,),
        in_specs=[at(first), at(first), at(first), at(first_dx)] + [whole(w) for w in weights],
        out_specs=[at()] * 2,
        out_shape=[jax.ShapeDtypeStruct((rows, d_model), F32)] * 2,
        scratch_shapes=[pltpu.VMEM((tile, d_ff), BF16)] * 3,
        compiler_params=params(60),
        cost_estimate=cost(12 * rows * d_model * d_ff, 6 * d_model * d_ff + 20 * rows * d_model, rows * d_ff),
        name="ffn_pair",
    )(x, c, y_in, dx_in, *weights)


def unset(*shapes):
    return pl.pallas_call(
        lambda *refs: None,
        out_specs=[pl.BlockSpec(memory_space=pl.ANY)] * len(shapes),
        out_shape=[jax.ShapeDtypeStruct(shape, BF16) for shape in shapes],
        name="unset",
    )()


def home_kernel(win, n_far, start_ref, near_ref, *refs):
    fars, (more_ref, out_ref, sum_ref) = refs[:n_far], refs[n_far:]
    row = 0
    for far in fars:
        rows = far.shape[0]
        sum_ref[row : row + rows, :] = (near_ref[row : row + rows, :] + far[...]).astype(BF16).astype(F32)
        row += rows
    sum_ref[row : row + more_ref.shape[0], :] = more_ref[...].astype(F32)
    row += more_ref.shape[0]
    sum_ref[row:, :] = jnp.zeros((sum_ref.shape[0] - row, sum_ref.shape[1]), F32)
    out_rows = out_ref.shape[1]
    to = lax.broadcasted_iota(jnp.int32, (out_rows, win), 0)
    frm = lax.broadcasted_iota(jnp.int32, (out_rows, win), 1)

    def block(o, _):
        start = start_ref[o]
        base = pl.multiple_of(start // 8 * 8, 8)
        rows = sum_ref[pl.ds(base, win), :].astype(BF16)
        move = one_hot(frm == to + (start - base))
        out_ref[o] = mm(move, rows).astype(BF16)
        return 0

    lax.fori_loop(0, out_ref.shape[0], block, 0)


def home_blocks(starts, near, fars, more, out_rows):
    n_out = starts.shape[0]
    d_model = near.shape[1]
    win = out_rows + 8
    vmem = pl.BlockSpec(memory_space=pltpu.VMEM)
    return pl.pallas_call(
        functools.partial(home_kernel, win, len(fars)),
        in_specs=[pl.BlockSpec(memory_space=pltpu.SMEM)] + [vmem] * (2 + len(fars)),
        out_specs=vmem,
        out_shape=jax.ShapeDtypeStruct((n_out, out_rows, d_model), BF16),
        scratch_shapes=[pltpu.VMEM((near.shape[0] + more.shape[0] + win, d_model), F32)],
        compiler_params=pltpu.CompilerParams(vmem_limit_bytes=58 * MIB),
        cost_estimate=cost(2 * n_out * out_rows * win * d_model, 12 * near.size),
        name="home_blocks",
    )(starts, near, *fars, more)


def return_kernel(n_etp, start_ref, first_ref, near_ref, far_ref, more_ref, part_ref, slot_ref, out_ref, total_ref, sum_ref, send_ref, back_ref, z_part, col_part, col_sum, send_sem, back_sem, z_sem, col_sem):
    t = lax.axis_index("etp")
    o = lax.axis_index("ep")
    n_ep = send_ref.shape[0]

    def col_at(i):
        col = o
        for bit in (1, 2, 4):
            if i & bit:
                col = flip_col(col, bit)
        return col

    barrier = pltpu.get_barrier_semaphore()
    planes = [(t + k) % n_etp for k in range(1, n_etp)]
    for i in range(1, n_ep):
        pl.semaphore_signal(barrier, device_id={"ep": col_at(i)}, device_id_type=pl.DeviceIdType.MESH)
    for plane in planes:
        pl.semaphore_signal(barrier, device_id={"etp": plane}, device_id_type=pl.DeviceIdType.MESH)
    pl.semaphore_wait(barrier, n_ep - 1 + n_etp - 1)

    def to(src, dst, sem, got, peer):
        return pltpu.make_async_remote_copy(src_ref=src, dst_ref=dst, send_sem=sem, recv_sem=got, device_id=peer, device_id_type=pl.DeviceIdType.MESH)

    z_copies = [to(part_ref, z_part.at[t], z_sem.at[0, k], z_sem.at[1, t], {"etp": plane}) for k, plane in enumerate(planes)]
    for copy in z_copies:
        copy.start()

    rows = first_ref.shape[0]
    sum_ref[:rows, :] = first_ref[...]
    end = rows + far_ref.shape[0]
    sum_ref[rows:end, :] = (near_ref[...] + far_ref[...]).astype(BF16)
    sum_ref[end:, :] = more_ref[...]

    blk_rows = send_ref.shape[1]
    put = lax.broadcasted_iota(jnp.int32, (blk_rows, sum_ref.shape[0]), 0)
    frm = lax.broadcasted_iota(jnp.int32, (blk_rows, sum_ref.shape[0]), 1)
    order = [6, 7, 2, 4, 3, 5, 1, 0]
    copies = {i: to(send_ref.at[i], back_ref.at[o], send_sem.at[i], back_sem.at[o], {"ep": col_at(i)}) for i in order if i}
    for k, i in enumerate(order):
        move = one_hot(frm == put + start_ref[col_at(i)])
        block = mm(move, sum_ref[...]).astype(BF16)
        if i:
            send_ref[i] = block
        else:
            back_ref[o] = block
        if k:
            copies[order[k - 1]].start()

    z_part[t] = part_ref[...]
    for plane in planes:
        to(part_ref, z_part.at[plane], z_sem.at[0, 0], z_sem.at[1, plane], {"etp": plane}).wait_recv()
    total = z_part[0]
    for k in range(1, n_etp):
        total += z_part[k]
    col_sum[...] = total

    cols = lax.broadcasted_iota(jnp.int32, (slot_ref.shape[0], blk_rows), 1)
    acc = jnp.zeros(out_ref.shape, F32)
    col_copies = {i: to(col_sum, col_part.at[o], col_sem.at[0, i], col_sem.at[1, o], {"ep": col_at(i)}) for i in range(1, n_ep)}
    for k, i in enumerate((0, 1, 2, 4, 3, 5, 6, 7)):
        col = col_at(i)
        if i:
            to(send_ref.at[i], back_ref.at[col], send_sem.at[i], back_sem.at[col], {"ep": col}).wait_recv()
        local = cols + col * blk_rows
        hit = (slot_ref[:, 0:1] == local) | (slot_ref[:, 1:2] == local)
        acc += mm(one_hot(hit), back_ref[col])
        if k == 1:
            for copy in col_copies.values():
                copy.start()
    out_ref[...] = acc

    col_part[o] = col_sum[...]
    for i in range(1, n_ep):
        col = col_at(i)
        to(col_sum, col_part.at[col], col_sem.at[0, i], col_sem.at[1, col], {"ep": col}).wait_recv()
    total = col_part[0]
    for k in range(1, n_ep):
        total += col_part[k]
    total_ref[...] = total
    for copy in [*z_copies, *copies.values(), *col_copies.values()]:
        copy.wait_send()


def return_rows(starts, first, near, far, more, part, slots, n_etp, n_ep, blk_rows):
    d_model = near.shape[1]
    out = jax.ShapeDtypeStruct((slots.shape[0], d_model), F32)
    half = far.shape[0]
    dma = pltpu.SemaphoreType.DMA
    vmem = lambda array: rows_at(*array.shape)
    blocks = pltpu.VMEM((n_ep, blk_rows, d_model), BF16)
    return pl.pallas_call(
        functools.partial(return_kernel, n_etp),
        grid=(1,),
        in_specs=[pl.BlockSpec(memory_space=pltpu.SMEM), vmem(first), rows_at(half, d_model, 1), vmem(far), vmem(more), vmem(part), vmem(slots)],
        out_specs=[vmem(out), vmem(part)],
        out_shape=[out, jax.ShapeDtypeStruct(part.shape, F32)],
        scratch_shapes=[
            pltpu.VMEM((2 * half + more.shape[0], d_model), BF16),
            blocks,
            blocks,
            pltpu.VMEM((n_etp, *part.shape), F32),
            pltpu.VMEM((n_ep, *part.shape), F32),
            pltpu.VMEM(part.shape, F32),
            dma((n_ep,)),
            dma((n_ep,)),
            dma((2, n_etp)),
            dma((2, n_ep)),
        ],
        compiler_params=pltpu.CompilerParams(collective_id=1, has_side_effects=True, vmem_limit_bytes=56 * MIB),
        cost_estimate=cost(10**10, 12 * near.size),
        name="return_rows",
    )(starts, first, near, far, more, part, slots)


def split3(value):
    high = lax.reduce_precision(value, 8, 7)
    rest = value - high
    mid = lax.reduce_precision(rest, 8, 7)
    return high.astype(BF16), mid.astype(BF16), (rest - mid).astype(BF16)


def solution(mesh):
    ep_size = mesh.shape["ep"]
    etp_size = mesh.shape["etp"]
    n_dev = ep_size * etp_size
    tok_spec = P(ALL_AXES, None)
    gate_spec = P("ep", None, "etp")
    down_spec = P("ep", "etp", None)

    def layer(hidden, w_router, expert_ids, d_out, w_gate, w_up, w_down):
        tok_rows, d_model = hidden.shape
        n_experts = w_router.shape[1]
        n_tokens = tok_rows * n_dev
        capacity = (5 * n_tokens + 2 * n_experts - 1) // (2 * n_experts)
        per_expert = 7 * tok_rows // (2 * n_experts)
        list_max = ep_size * per_expert
        main_rows = 23 * tok_rows // 8
        more_rows = list_max - main_rows
        tile = main_rows // 4
        win = per_expert + 8
        ep_i = lax.axis_index("ep")
        etp_i = lax.axis_index("etp")
        block_idx = ep_i * etp_size + etp_i
        w1, w3, w2 = w_gate[0], w_up[0], w_down[0]

        def swap(array, even, odd):
            pairs = [(t * ep_size + o, (odd if o % 2 else even)[t] * ep_size + o) for t in range(etp_size) for o in range(ep_size)]
            return lax.ppermute(array, ("etp", "ep"), pairs)

        ids_row = expert_ids.T.astype(BF16).reshape(1, 2 * tok_rows)
        ids_row = jnp.concatenate([ids_row, jnp.zeros((7, 2 * tok_rows), BF16)])
        h_all, dy_col = spread_all(jnp.concatenate([hidden, ids_row]), d_out, etp_size, ep_size)
        w1_b, w3_b, w2_b, h_all, dy_b = lax.optimization_barrier((w1, w3, w2, h_all, dy_col))
        w1p = swap(w1_b, NEXT_PAIRS, ENDS_PAIRS)
        w3p = swap(w3_b, NEXT_PAIRS, ENDS_PAIRS)
        w2p = swap(w2_b, NEXT_PAIRS, ENDS_PAIRS)

        def flip(array, bit):
            return lax.ppermute(array, "ep", [(o, o ^ bit) for o in range(ep_size)])

        half_z = etp_size // 2
        dy_c, dy_x, dy_y = [flip(dy_b, bit) for bit in (1, 2, 4)]
        dy_d = flip(dy_y[:half_z], 2), flip(dy_x[half_z:], 4)
        dy_cx, dy_cy = flip(dy_x, 1), flip(dy_y, 1)
        dy_d = jnp.concatenate(dy_d)
        dy_cd = flip(dy_d, 1)
        dy_all = [dy_b, dy_c, dy_x, dy_cx, dy_y, dy_cy, dy_d, dy_cd]
        dy_cols = (ep_i ^ jnp.arange(ep_size)).astype(jnp.int32)
        all_cols = jnp.arange(ep_size, dtype=jnp.int32)

        ids_all = h_all[:, tok_rows, :].astype(jnp.int32).reshape(n_dev, 2, tok_rows)
        id0, id1 = ids_all[:, 0], ids_all[:, 1]
        experts = jnp.arange(n_experts, dtype=jnp.int32)[None, :, None]
        count = jnp.sum(((id0[:, None, :] == experts) | (id1[:, None, :] == experts)).astype(F32), axis=2)
        before = jnp.cumsum(count, axis=0) - count
        kept = jnp.clip(capacity - before, 0, count).astype(jnp.int32)
        kept_lists = kept.reshape(ep_size, etp_size, n_experts)
        list_start = jnp.cumsum(kept_lists, axis=0) - kept_lists
        list_len = jnp.sum(kept_lists, axis=0)
        earlier = (jnp.arange(tok_rows)[:, None] < jnp.arange(tok_rows)[None, :]).astype(BF16)

        my_member = (id0 == ep_i) | (id1 == ep_i)
        my_rank = mm(my_member.astype(BF16), earlier).astype(jnp.int32)
        my_start = lax.dynamic_index_in_dim(list_start, ep_i, 2, keepdims=False)
        my_kept = lax.dynamic_index_in_dim(kept, ep_i, 1, keepdims=True)
        my_pos = jnp.where(my_member & (my_rank < my_kept), my_start.reshape(n_dev, 1) + my_rank, -1)
        odd = ep_i % 2
        far = jnp.where(odd == 1, etp_i ^ 1, etp_size - 1 - etp_i)
        planes = jnp.stack([far, etp_i, far ^ 2, etp_i ^ 2]).astype(jnp.int32)
        my_base = jnp.minimum(my_start, main_rows) // 8 * 8
        pick = functools.partial(pick_rows, win=win, n_src=ep_size, n_etp=etp_size)
        main_pos = jnp.where(my_pos < main_rows, my_pos, -1)
        main_base = my_base.T[planes]
        x_main = pick([h_all], all_cols, main_pos, None, planes, main_base, main_rows)

        route_w = jnp.concatenate(split3(w_router), axis=1)
        logit_parts = lax.dot_general(route_w, h_all, (((0,), (2,)), ((), ())), preferred_element_type=F32)[:, :, :tok_rows].reshape(-1, n_tokens)
        logits = logit_parts[:n_experts] + logit_parts[n_experts : 2 * n_experts] + logit_parts[2 * n_experts :]
        probs_all = jax.nn.softmax(logits, axis=0)
        expert_col = jnp.arange(n_experts, dtype=jnp.int32)[:, None]
        picked_all = jnp.where((id0.reshape(1, -1) == expert_col) | (id1.reshape(1, -1) == expert_col), probs_all, 0.0)
        my_gate = lax.dynamic_index_in_dim(picked_all, ep_i, 0, keepdims=False) / jnp.sum(picked_all, axis=0)
        mean_prob = jnp.sum(probs_all, axis=1) / n_tokens
        my_scale = OUT_SCALE * my_gate.reshape(n_dev, tok_rows)
        c_main = pick(dy_all, dy_cols, main_pos, my_scale, planes, main_base, main_rows)

        n_rows = x_main.shape[0]
        *acts, y_base = ffn_act(x_main, (w1, w3, w2), tile, 0, 8, (), n_rows)
        act_a, act_b, inner = ffn_act(x_main, (w1, w3), tile, 8, 8, acts, n_rows)
        far_a, far_b, far_u = ffn_act(x_main, (w1p, w3p), tile, 0, 4, (), main_rows)
        *grads, dx_base = ffn_grad(c_main, act_a, act_b, (w2, w1, w3), tile, 0, 0, 4, (), n_rows)
        y_far, dx_far = [], []
        for i, n_tiles in enumerate((1, 3)):
            y_part = ffn_down(far_u, w2p, y_base, tile, i, n_tiles)
            y_far.append(swap(y_part, ENDS_PAIRS, NEXT_PAIRS))
        for i in range(2):
            (dx_part,) = ffn_grad(c_main, far_a, far_b, (w2p, w1p, w3p), tile, 2 * i, 2 * i, 2, (), base=(dx_base,))
            dx_far.append(swap(dx_part, ENDS_PAIRS, NEXT_PAIRS))
        grads = ffn_grad(c_main, act_a, act_b, (w2, w1, w3), tile, 4, 4, 2, grads, n_rows, dx_rows=main_rows)
        *grads, dx_base = ffn_grad(c_main, act_a, act_b, (w2, w1, w3), tile, 6, 6, 2, grads, n_rows, dx_rows=main_rows, first_dx=2)
        y_near, dx_near = ffn_pair(x_main, c_main, y_base, dx_base, (w1p, w3p, w2p), tile, 4, 4, 0)
        d_a, d_b = ffn_grad(c_main, act_a, act_b, (w2,), tile, 8, 8, 8, grads, n_rows)

        def add_planes(parts):
            total = parts[etp_i]
            for k in range(1, etp_size):
                shift = [(t, (t + k) % etp_size) for t in range(etp_size)]
                total += lax.ppermute(parts[(etp_i + k) % etp_size], "etp", shift)
            return total

        def more_work(*_):
            more_pos = jnp.where(my_pos >= main_rows, my_pos - main_rows, -1)
            more_base = jnp.clip(my_start.T - main_rows, 0, more_rows) // 8 * 8
            order = jnp.arange(etp_size, dtype=jnp.int32)
            x_more = pick([h_all], all_cols, more_pos, None, order, more_base, more_rows)
            c_more = pick(dy_all, dy_cols, more_pos, my_scale, order, more_base, more_rows)
            act_a, act_b, inner, y_part = ffn_act(x_more, (w1, w3, w2), more_rows, 0, etp_size, (), n_more)
            d_a, d_b, dx_part = ffn_grad(c_more, act_a, act_b, (w2, w1, w3), more_rows, 0, 0, etp_size, (), n_more)
            sums = [add_planes(part.reshape(etp_size, more_rows, d_model)).astype(BF16) for part in (y_part, dx_part)]
            return *sums, x_more, c_more, inner, d_a, d_b

        n_more = etp_size * more_rows
        none = jnp.zeros((more_rows, d_model), BF16)
        spare = none, none, *unset(*[(n_more, d_model)] * 2, *[(n_more, w1.shape[1])] * 3)
        any_more = jnp.max(list_len) > main_rows
        y_more, dx_more, x_more, c_more, *more_acts = lax.cond(any_more, more_work, lambda *spare: spare, *spare)

        def more_grads(*grads):
            inner_more, d_a_more, d_b_more = more_acts
            return grads[0] + mm_tn(x_more, d_a_more), grads[1] + mm_tn(x_more, d_b_more), grads[2] + mm_tn(inner_more, c_more)

        home_start = lax.dynamic_index_in_dim(my_start, etp_i, 1, keepdims=False)

        hot = [(expert_ids[:, k : k + 1] == experts[0].T).astype(F32) for k in range(2)]
        probs = lax.dynamic_slice_in_dim(probs_all, block_idx * tok_rows, tok_rows, 1).T
        picked = [jnp.sum(probs * hot[k], axis=1, keepdims=True) for k in range(2)]
        pick_sum = picked[0] + picked[1]
        gates = [picked[k] / pick_sum for k in range(2)]
        my_kept_row = lax.dynamic_index_in_dim(kept, block_idx, 0, keepdims=True).astype(F32)
        rank = mm_tn(earlier, (hot[0] + hot[1]).astype(BF16))
        slot_row = jnp.arange(n_experts * per_expert, dtype=jnp.int32)[None, :]
        slots, chosen = [], []
        for k in range(2):
            rank_k = jnp.sum(rank * hot[k], axis=1, keepdims=True)
            kept_k = jnp.sum(my_kept_row * hot[k], axis=1, keepdims=True)
            slot_k = jnp.where(rank_k < kept_k, expert_ids[:, k : k + 1] * per_expert + rank_k.astype(jnp.int32), -1)
            slots.append(slot_k)
            chosen.append(slot_k == slot_row)

        dw1 = mm_tn(x_main, d_a)
        y_near, dw1, x_main = lax.optimization_barrier((y_near, dw1, x_main))
        y_back = home_blocks(home_start, y_near, y_far, y_more, per_expert)
        y_back = lax.all_to_all(y_back, "ep", 0, 0, tiled=True).reshape(n_experts * per_expert, d_model)
        dw3 = mm_tn(x_main, d_b)
        dw2 = mm_tn(inner, c_main)
        dw1, dw3, dw2 = lax.cond(any_more, more_grads, lambda *grads: grads, dw1, dw3, dw2)
        y_pair = [mm(chosen[k].astype(BF16), y_back) for k in range(2)]
        hidden_f = hidden.astype(F32)
        output = (hidden_f + OUT_SCALE * (gates[0] * y_pair[0] + gates[1] * y_pair[1])).astype(BF16)
        d_out_f = d_out.astype(F32)
        d_gates = [jnp.sum(OUT_SCALE * d_out_f * y_pair[k], axis=1, keepdims=True) for k in range(2)]

        route_frac = jnp.sum(count, axis=0) / (2 * n_tokens)
        aux_loss = AUX_COEF * n_experts * jnp.sum(route_frac * mean_prob)
        mix = gates[0] * d_gates[0] + gates[1] * d_gates[1]
        d_probs = (AUX_COEF * n_experts / n_tokens) * route_frac[None, :]
        for k in range(2):
            d_probs = d_probs + hot[k] * ((d_gates[k] - mix) / pick_sum)
        d_logits = probs * (d_probs - jnp.sum(probs * d_probs, axis=1, keepdims=True))
        d_router_part = mm_tn(d_logits, hidden_f, lax.Precision.HIGHEST)
        d_route = mm_nt(d_logits, w_router, lax.Precision.HIGHEST)
        rest = d_out_f + d_route
        rest, first_far = lax.optimization_barrier((rest, dx_far[0]))
        first_dx = (dx_near[: main_rows // 2] + first_far).astype(BF16)
        dx_near, dw1, dw3, dw2, rest, first_dx, output = lax.optimization_barrier((dx_near, dw1, dw3, dw2, rest, first_dx, output))
        dx_sum, d_router = return_rows(home_start, first_dx, dx_near, dx_far[1], dx_more, d_router_part, jnp.concatenate(slots, axis=1), etp_size, ep_size, per_expert)
        d_hidden = (rest + dx_sum).astype(BF16)
        d_router = d_router.T
        return output, d_hidden, d_router, aux_loss, dw1[None], dw3[None], dw2[None]

    return jax.shard_map(layer, mesh=mesh, in_specs=(tok_spec, P(), tok_spec, tok_spec, gate_spec, gate_spec, down_spec), out_specs=(tok_spec, tok_spec, P(), P(), gate_spec, gate_spec, down_spec), check_vma=False)
```

```python
import functools
import jax
import jax.numpy as jnp
from jax import lax
from jax.experimental import pallas as pl
from jax.experimental.pallas import tpu as pltpu
from jax.sharding import PartitionSpec as P


AUX_COEF = 0.01
OUT_SCALE = 2.0
ALL_AXES = ("ep", "etp")
BF16 = jnp.bfloat16
F32 = jnp.float32
MIB = 1 << 20
FF_STEP = 256

NEXT_PAIRS = (1, 0, 3, 2)
ENDS_PAIRS = (3, 2, 1, 0)


def mm(lhs, rhs):
    return jnp.dot(lhs, rhs, preferred_element_type=F32)


def mm_nt(lhs, rhs, precision=None):
    return lax.dot_general(lhs, rhs, (((1,), (1,)), ((), ())), precision=precision, preferred_element_type=F32)


def mm_tn(lhs, rhs, precision=None):
    return lax.dot_general(lhs, rhs, (((0,), (0,)), ((), ())), precision=precision, preferred_element_type=F32)


def params(vmem_mib):
    return pltpu.CompilerParams(dimension_semantics=("arbitrary",), vmem_limit_bytes=vmem_mib * MIB)


def cost(flops, bytes_accessed, transcendentals=0):
    return pl.CostEstimate(flops=flops, bytes_accessed=bytes_accessed, transcendentals=transcendentals)


def rows_at(rows, width, start=0):
    return pl.BlockSpec((rows, width), lambda i: (i + start, 0))


def by_columns(width, step):
    def at(i, carry):
        step(pl.ds(pl.multiple_of(i * FF_STEP, FF_STEP), FF_STEP))
        return carry

    lax.fori_loop(0, width // FF_STEP, at, 0, unroll=True)


def flip_col(col, bit):
    return col + bit * (1 - 2 * ((col // bit) % 2))


def one_hot(hit):
    return hit.astype(F32).astype(BF16)


def spread_kernel(n_etp, h_ref, dy_ref, h_all, dy_col, h_recv, dy_recv, z_send, x_send, y_send, c_send, own_sem):
    t = lax.axis_index("etp")
    o = lax.axis_index("ep")
    col_c, col_x, col_y = [flip_col(o, bit) for bit in (1, 2, 4)]
    col_d = flip_col(col_x, 4)
    order = [t, flip_col(t, 1), flip_col(t, 2), n_etp - 1 - t]
    has_left, has_right = t > 0, t < n_etp - 1

    barrier = pltpu.get_barrier_semaphore()
    for col in (col_c, col_x, col_y):
        pl.semaphore_signal(barrier, device_id={"ep": col}, device_id_type=pl.DeviceIdType.MESH)

    @pl.when(has_left)
    def _():
        pl.semaphore_signal(barrier, device_id={"etp": t - 1}, device_id_type=pl.DeviceIdType.MESH)

    @pl.when(has_right)
    def _():
        pl.semaphore_signal(barrier, device_id={"etp": t + 1}, device_id_type=pl.DeviceIdType.MESH)

    pl.semaphore_wait(barrier, 3 + (t + n_etp - 1) // n_etp + (2 * n_etp - 2 - t) // n_etp)

    keep = [pltpu.make_async_copy(h_ref, h_all.at[o * n_etp + t], own_sem.at[0]), pltpu.make_async_copy(dy_ref, dy_col.at[t], own_sem.at[1])]
    for copy in keep:
        copy.start()

    def h_copy(col, s, send_sem, to):
        slot = col * n_etp + s
        return pltpu.make_async_remote_copy(src_ref=h_all.at[slot], dst_ref=h_all.at[slot], send_sem=send_sem, recv_sem=h_recv.at[slot], device_id=to, device_id_type=pl.DeviceIdType.MESH)

    def own_copy(send_sem, to):
        slot = o * n_etp + t
        return pltpu.make_async_remote_copy(src_ref=h_ref, dst_ref=h_all.at[slot], send_sem=send_sem, recv_sem=h_recv.at[slot], device_id=to, device_id_type=pl.DeviceIdType.MESH)

    def dy_copy(s, send_sem, to, own=False):
        return pltpu.make_async_remote_copy(src_ref=dy_ref if own else dy_col.at[s], dst_ref=dy_col.at[s], send_sem=send_sem, recv_sem=dy_recv.at[s], device_id=to, device_id_type=pl.DeviceIdType.MESH)

    def h_arrived(col, s):
        h_copy(col, s, own_sem.at[0], {"ep": col_c}).wait_recv()

    def dy_arrived(s):
        dy_copy(s, own_sem.at[0], {"ep": col_c}).wait_recv()

    right, left = {"etp": t + 1}, {"etp": t - 1}
    to_x, to_y, to_c = {"ep": col_x}, {"ep": col_y}, {"ep": col_c}

    def z_copy(k, data, go):
        s, to, sem = (t - k, right, z_send.at[data, 0, k]) if go == 0 else (t + k, left, z_send.at[data, 1, k])
        if data == 0:
            return own_copy(sem, to) if k == 0 else h_copy(o, s, sem, to)
        return dy_copy(s, sem, to, own=k == 0)

    def z_goes(k, go):
        return has_right & (t >= k) if go == 0 else has_left & (t <= n_etp - 1 - k)

    def z_send_step(k, data):
        for go in (0, 1):
            pl.when(z_goes(k, go))(lambda: z_copy(k, data, go).start())

    def z_arrive(k, data):
        arrived = (lambda s: h_arrived(o, s)) if data == 0 else dy_arrived
        pl.when(t >= k)(lambda: arrived(t - k))
        pl.when(t <= n_etp - 1 - k)(lambda: arrived(t + k))

    def a_step(k):
        s = order[k]
        for sem, to in ((x_send.at[k], to_x), (y_send.at[k], to_y), (c_send.at[0, k], to_c)):
            (own_copy(sem, to) if k == 0 else h_copy(o, s, sem, to)).start()

    def b_step(k):
        s = order[k]
        h_arrived(col_x, s)
        if k % 2 == 0:
            h_copy(col_x, s, y_send.at[4 + k // 2], to_y).start()
        h_copy(col_x, s, c_send.at[1, k], to_c).start()
        h_arrived(col_y, s)
        if k % 2 == 1:
            h_copy(col_y, s, x_send.at[4 + k // 2], to_x).start()
        h_copy(col_y, s, c_send.at[2, k], to_c).start()

    def c_step(k):
        s = order[k]
        h_arrived(col_d, s)
        h_copy(col_d, s, c_send.at[3, k], to_c).start()

    steps = {
        "s": functools.partial(z_send_step, data=0),
        "S": functools.partial(z_send_step, data=1),
        "r": functools.partial(z_arrive, data=0),
        "R": functools.partial(z_arrive, data=1),
        "a": a_step,
        "b": b_step,
        "c": c_step,
    }
    plan = "s0a0r1s1a1b0r2s2S0a2b1r3a3c0b2c1R1S1b3R2S2c2c3R3"
    for kind, k in zip(plan[::2], plan[1::2]):
        steps[kind](int(k))

    for k in range(n_etp):
        for col in (col_x, col_y, col_d):
            h_arrived(flip_col(col, 1), order[k])
        h_arrived(col_c, order[k])
    for copy in keep:
        copy.wait()
    for k in range(n_etp - 1):
        for data in (0, 1):
            for go in (0, 1):
                pl.when(z_goes(k, go))(lambda: z_copy(k, data, go).wait_send())
    for i in range(6):
        h_copy(o, t, x_send.at[i], to_x).wait_send()
        h_copy(o, t, y_send.at[i], to_y).wait_send()
    for j in range(4):
        for k in range(n_etp):
            h_copy(o, t, c_send.at[j, k], to_c).wait_send()


def spread_all(h, dy, n_etp, n_ep):
    hbm = pl.BlockSpec(memory_space=pl.ANY)
    vmem = pl.BlockSpec(memory_space=pltpu.VMEM)
    dma = pltpu.SemaphoreType.DMA
    return pl.pallas_call(
        functools.partial(spread_kernel, n_etp),
        in_specs=[vmem, vmem],
        out_specs=[hbm, hbm],
        out_shape=[jax.ShapeDtypeStruct((n_ep * n_etp, *h.shape), h.dtype), jax.ShapeDtypeStruct((n_etp, *dy.shape), dy.dtype)],
        scratch_shapes=[dma((n_ep * n_etp,)), dma((n_etp,)), dma((2, 2, n_etp - 1)), dma((6,)), dma((6,)), dma((4, n_etp)), dma((2,))],
        compiler_params=pltpu.CompilerParams(collective_id=0, has_side_effects=True, vmem_limit_bytes=16 * MIB),
        cost_estimate=cost(10**11, 2 * n_ep * n_etp * h.size),
        name="spread_all",
    )(h, dy)


def pick_kernel(n_arrays, scaled, win, planes_ref, cols_ref, base_ref, *refs):
    sources, (pos_ref, *gate_ref, out_ref, acc_ref) = refs[:n_arrays], refs[n_arrays:]
    grp = pl.program_id(0)
    acc_ref[...] = jnp.zeros_like(acc_ref)
    for i in range(pos_ref.shape[0]):
        col = cols_ref[i]
        base = pl.multiple_of(base_ref[grp, col], 8)
        pos_row = pos_ref[col, 0]
        want = base + lax.broadcasted_iota(jnp.int32, (win, pos_row.shape[1]), 0)
        hit = want == pos_row
        block = sources[i][0] if n_arrays > 1 else sources[0][i, 0]
        part = mm(one_hot(hit), block)
        if scaled:
            part = part * jnp.sum(jnp.where(hit, gate_ref[0][col, 0], 0.0), axis=1, keepdims=True)
        acc_ref[pl.ds(base, win), :] += part
    out_ref[...] = acc_ref[: out_ref.shape[0], :].astype(out_ref.dtype)


def pick_rows(sources, cols, pos, gates, planes, base, n_rows, win, n_src, n_etp):
    blk_rows = pos.shape[-1]
    d_model = sources[0].shape[-1]
    n_grp = planes.shape[0]
    plane_map = lambda g, planes, cols, base: (0, planes[g], 0, 0)
    table_spec = pl.BlockSpec((n_src, 1, 1, blk_rows), plane_map)
    if len(sources) == 1:
        sources = [sources[0].reshape(n_src, n_etp, *sources[0].shape[1:])]
        source_spec = pl.BlockSpec((n_src, 1, blk_rows, d_model), plane_map)
    else:
        source_spec = pl.BlockSpec((1, blk_rows, d_model), lambda g, planes, cols, base: (planes[g], 0, 0))
    tables = [table.reshape(n_src, n_etp, 1, blk_rows) for table in (pos, gates) if table is not None]
    work = n_grp * n_src * blk_rows * d_model
    return pl.pallas_call(
        functools.partial(pick_kernel, len(sources), gates is not None, win),
        grid_spec=pltpu.PrefetchScalarGridSpec(
            num_scalar_prefetch=3,
            grid=(n_grp,),
            in_specs=[source_spec] * len(sources) + [table_spec] * len(tables),
            out_specs=pl.BlockSpec((n_rows, d_model), lambda g, planes, cols, base: (g, 0)),
            scratch_shapes=[pltpu.VMEM((n_rows + win, d_model), F32)],
        ),
        out_shape=jax.ShapeDtypeStruct((n_grp * n_rows, d_model), BF16),
        compiler_params=params(58),
        cost_estimate=cost(2 * win * work, 4 * work),
        name="pick_rows",
    )(planes, cols, base, *sources, *tables)


def whole(array):
    return pl.BlockSpec(array.shape, lambda i: (0, 0), pipeline_mode=pl.Buffered(1))


def sum_into(out_ref, base_ref, product):
    def step(cols):
        part = product(cols)
        out_ref[:, cols] = part if base_ref is None else base_ref[:, cols] + part

    by_columns(out_ref.shape[1], step)


def act_kernel(with_y, n_alias, x_ref, *refs):
    (w1, w3, *w2), refs = refs[: 2 + with_y], refs[2 + with_y + n_alias :]
    a_ref, b_ref, u_ref = refs[:3]

    def step(cols):
        act_a = mm(x_ref[...], w1[:, cols])
        act_b = mm(x_ref[...], w3[:, cols])
        a_ref[:, cols] = act_a
        b_ref[:, cols] = act_b
        u_ref[:, cols] = (act_a * jax.nn.sigmoid(act_a) * act_b).astype(BF16)

    by_columns(w1.shape[1], step)
    if with_y:
        sum_into(refs[3], None, lambda cols: mm(u_ref[...], w2[0][:, cols]))


def ffn_act(x, weights, tile, first, n_tiles, kept, total):
    d_model, d_ff = weights[0].shape
    with_y = len(weights) == 3
    rows = n_tiles * tile
    out_specs = [rows_at(tile, d_ff, first)] * 3
    out_shape = [jax.ShapeDtypeStruct((total, d_ff), dtype) for dtype in (F32, F32, BF16)]
    if with_y:
        out_specs.append(rows_at(tile, d_model))
        out_shape.append(jax.ShapeDtypeStruct((rows, d_model), F32))
    n_in = 1 + len(weights)
    return pl.pallas_call(
        functools.partial(act_kernel, with_y, len(kept)),
        grid=(n_tiles,),
        in_specs=[rows_at(tile, d_model, first)] + [whole(w) for w in weights] + [pl.BlockSpec(memory_space=pl.ANY)] * len(kept),
        out_specs=out_specs,
        out_shape=out_shape,
        input_output_aliases={n_in + i: i for i in range(len(kept))},
        compiler_params=params(60),
        cost_estimate=cost(2 * len(weights) * rows * d_model * d_ff, 6 * d_model * d_ff + 10 * rows * d_ff, rows * d_ff),
        name="ffn_act",
    )(x, *weights, *kept)


def down_kernel(u_ref, w2, y_in, y_ref):
    sum_into(y_ref, y_in, lambda cols: mm(u_ref[...], w2[:, cols]))


def ffn_down(u, w2, y_in, tile, first, n_tiles):
    d_ff, d_model = w2.shape
    rows = n_tiles * tile
    return pl.pallas_call(
        down_kernel,
        grid=(n_tiles,),
        in_specs=[rows_at(tile, d_ff, first), whole(w2), rows_at(tile, d_model, first)],
        out_specs=rows_at(tile, d_model),
        out_shape=jax.ShapeDtypeStruct((rows, d_model), F32),
        compiler_params=params(48),
        cost_estimate=cost(2 * rows * d_model * d_ff, 2 * d_model * d_ff + 8 * rows * d_model),
        name="ffn_down",
    )(u, w2, y_in)


def grad_kernel(with_dx, keeps, n_base, n_alias, c_ref, a_ref, b_ref, *refs):
    n_w = 3 if with_dx else 1
    (w2, *w13), base, refs = refs[:n_w], refs[n_w : n_w + n_base], list(refs[n_w + n_base + n_alias :])
    dx_ref = refs.pop(2 if keeps else 0) if with_dx else None
    da_ref, db_ref = refs

    def step(cols):
        d_inner = mm_nt(c_ref[...], w2[cols, :])
        act_a = a_ref[:, cols]
        sig_a = jax.nn.sigmoid(act_a)
        da_ref[:, cols] = (d_inner * b_ref[:, cols] * sig_a * (1.0 + act_a * (1.0 - sig_a))).astype(BF16)
        db_ref[:, cols] = (d_inner * (act_a * sig_a)).astype(BF16)

    by_columns(w2.shape[0], step)
    if with_dx:
        w1, w3 = w13
        sum_into(dx_ref, base[0] if base else None, lambda cols: mm_nt(da_ref[...], w1[cols, :]) + mm_nt(db_ref[...], w3[cols, :]))


def ffn_grad(c, act_a, act_b, weights, tile, first, first_act, n_tiles, kept, total=0, base=()):
    w2, *w13 = weights
    d_ff, d_model = w2.shape
    with_dx = bool(w13)
    rows = n_tiles * tile
    at = functools.partial(rows_at, tile)
    out_specs = [at(d_ff, first)] * 2 if total else []
    out_shape = [jax.ShapeDtypeStruct((total, d_ff), BF16)] * 2 if total else []
    if with_dx:
        out_specs.append(at(d_model))
        out_shape.append(jax.ShapeDtypeStruct((rows, d_model), F32))
    n_in = 3 + len(weights) + len(base)
    return pl.pallas_call(
        functools.partial(grad_kernel, with_dx, bool(total), len(base), len(kept)),
        grid=(n_tiles,),
        in_specs=[at(d_model, first), at(d_ff, first_act), at(d_ff, first_act)] + [whole(w) for w in weights] + [at(d_model, first)] * len(base) + [pl.BlockSpec(memory_space=pl.ANY)] * len(kept),
        out_specs=out_specs,
        out_shape=out_shape,
        scratch_shapes=[] if total else [pltpu.VMEM((tile, d_ff), BF16)] * 2,
        input_output_aliases={n_in + i: i for i in range(len(kept))},
        compiler_params=params(62),
        cost_estimate=cost(2 * len(weights) * rows * d_model * d_ff, 6 * d_model * d_ff + 12 * rows * d_ff, rows * d_ff),
        name="ffn_grad",
    )(c, act_a, act_b, *weights, *base, *kept)


def pair_kernel(x_ref, c_ref, y_in, dx_in, w1, w3, w2, y_ref, dx_ref, u_ref, da_ref, db_ref):
    def step(cols):
        act_a = mm(x_ref[...], w1[:, cols])
        act_b = mm(x_ref[...], w3[:, cols])
        d_inner = mm_nt(c_ref[...], w2[cols, :])
        sig_a = jax.nn.sigmoid(act_a)
        silu_a = act_a * sig_a
        u_ref[:, cols] = (silu_a * act_b).astype(BF16)
        da_ref[:, cols] = (d_inner * act_b * sig_a * (1.0 + act_a * (1.0 - sig_a))).astype(BF16)
        db_ref[:, cols] = (d_inner * silu_a).astype(BF16)

    by_columns(w1.shape[1], step)
    sum_into(y_ref, y_in, lambda cols: mm(u_ref[...], w2[:, cols]))
    sum_into(dx_ref, dx_in, lambda cols: mm_nt(da_ref[...], w1[cols, :]) + mm_nt(db_ref[...], w3[cols, :]))


def ffn_pair(x, c, y_in, dx_in, weights, tile, first, n_tiles, first_dx):
    d_model, d_ff = weights[0].shape
    rows = n_tiles * tile
    at = functools.partial(rows_at, tile, d_model)
    return pl.pallas_call(
        pair_kernel,
        grid=(n_tiles,),
        in_specs=[at(first), at(first), at(first), at(first_dx)] + [whole(w) for w in weights],
        out_specs=[at()] * 2,
        out_shape=[jax.ShapeDtypeStruct((rows, d_model), F32)] * 2,
        scratch_shapes=[pltpu.VMEM((tile, d_ff), BF16)] * 3,
        compiler_params=params(60),
        cost_estimate=cost(12 * rows * d_model * d_ff, 6 * d_model * d_ff + 20 * rows * d_model, rows * d_ff),
        name="ffn_pair",
    )(x, c, y_in, dx_in, *weights)


def unset(*shapes):
    return pl.pallas_call(
        lambda *refs: None,
        out_specs=[pl.BlockSpec(memory_space=pl.ANY)] * len(shapes),
        out_shape=[jax.ShapeDtypeStruct(shape, BF16) for shape in shapes],
        name="unset",
    )()


def home_kernel(win, n_far, start_ref, near_ref, *refs):
    fars, (more_ref, out_ref, sum_ref) = refs[:n_far], refs[n_far:]
    row = 0
    for far in fars:
        rows = far.shape[0]
        sum_ref[row : row + rows, :] = (near_ref[row : row + rows, :] + far[...]).astype(BF16).astype(F32)
        row += rows
    sum_ref[row : row + more_ref.shape[0], :] = more_ref[...].astype(F32)
    row += more_ref.shape[0]
    sum_ref[row:, :] = jnp.zeros((sum_ref.shape[0] - row, sum_ref.shape[1]), F32)
    out_rows = out_ref.shape[1]
    to = lax.broadcasted_iota(jnp.int32, (out_rows, win), 0)
    frm = lax.broadcasted_iota(jnp.int32, (out_rows, win), 1)

    def block(o, _):
        start = start_ref[o]
        base = pl.multiple_of(start // 8 * 8, 8)
        rows = sum_ref[pl.ds(base, win), :].astype(BF16)
        move = one_hot(frm == to + (start - base))
        out_ref[o] = mm(move, rows).astype(BF16)
        return 0

    lax.fori_loop(0, out_ref.shape[0], block, 0)


def home_blocks(starts, near, fars, more, out_rows):
    n_out = starts.shape[0]
    d_model = near.shape[1]
    win = out_rows + 8
    vmem = pl.BlockSpec(memory_space=pltpu.VMEM)
    return pl.pallas_call(
        functools.partial(home_kernel, win, len(fars)),
        in_specs=[pl.BlockSpec(memory_space=pltpu.SMEM)] + [vmem] * (2 + len(fars)),
        out_specs=vmem,
        out_shape=jax.ShapeDtypeStruct((n_out, out_rows, d_model), BF16),
        scratch_shapes=[pltpu.VMEM((near.shape[0] + more.shape[0] + win, d_model), F32)],
        compiler_params=pltpu.CompilerParams(vmem_limit_bytes=58 * MIB),
        cost_estimate=cost(2 * n_out * out_rows * win * d_model, 12 * near.size),
        name="home_blocks",
    )(starts, near, *fars, more)


def return_kernel(n_etp, start_ref, near_ref, far_ref, more_ref, part_ref, slot_ref, out_ref, total_ref, sum_ref, send_ref, back_ref, z_part, col_part, col_sum, send_sem, back_sem, z_sem, col_sem):
    t = lax.axis_index("etp")
    o = lax.axis_index("ep")
    n_ep = send_ref.shape[0]

    def col_at(i):
        col = o
        for bit in (1, 2, 4):
            if i & bit:
                col = flip_col(col, bit)
        return col

    barrier = pltpu.get_barrier_semaphore()
    planes = [(t + k) % n_etp for k in range(1, n_etp)]
    for i in range(1, n_ep):
        pl.semaphore_signal(barrier, device_id={"ep": col_at(i)}, device_id_type=pl.DeviceIdType.MESH)
    for plane in planes:
        pl.semaphore_signal(barrier, device_id={"etp": plane}, device_id_type=pl.DeviceIdType.MESH)
    pl.semaphore_wait(barrier, n_ep - 1 + n_etp - 1)

    def to(src, dst, sem, got, peer):
        return pltpu.make_async_remote_copy(src_ref=src, dst_ref=dst, send_sem=sem, recv_sem=got, device_id=peer, device_id_type=pl.DeviceIdType.MESH)

    z_copies = [to(part_ref, z_part.at[t], z_sem.at[0, k], z_sem.at[1, t], {"etp": plane}) for k, plane in enumerate(planes)]
    for copy in z_copies:
        copy.start()

    end = far_ref.shape[0]
    sum_ref[:end, :] = (near_ref[...] + far_ref[...]).astype(BF16)
    sum_ref[end:, :] = more_ref[...]

    blk_rows = send_ref.shape[1]
    put = lax.broadcasted_iota(jnp.int32, (blk_rows, sum_ref.shape[0]), 0)
    frm = lax.broadcasted_iota(jnp.int32, (blk_rows, sum_ref.shape[0]), 1)
    order = [6, 7, 2, 4, 3, 5, 1, 0]
    copies = {i: to(send_ref.at[i], back_ref.at[o], send_sem.at[i], back_sem.at[o], {"ep": col_at(i)}) for i in order if i}
    for k, i in enumerate(order):
        move = one_hot(frm == put + start_ref[col_at(i)])
        block = mm(move, sum_ref[...]).astype(BF16)
        if i:
            send_ref[i] = block
        else:
            back_ref[o] = block
        if k:
            copies[order[k - 1]].start()

    z_part[t] = part_ref[...]
    for plane in planes:
        to(part_ref, z_part.at[plane], z_sem.at[0, 0], z_sem.at[1, plane], {"etp": plane}).wait_recv()
    total = z_part[0]
    for k in range(1, n_etp):
        total += z_part[k]
    col_sum[...] = total

    cols = lax.broadcasted_iota(jnp.int32, (slot_ref.shape[0], blk_rows), 1)
    acc = jnp.zeros(out_ref.shape, F32)
    col_copies = {i: to(col_sum, col_part.at[o], col_sem.at[0, i], col_sem.at[1, o], {"ep": col_at(i)}) for i in range(1, n_ep)}
    for k, i in enumerate((0, 1, 2, 4, 3, 5, 6, 7)):
        col = col_at(i)
        if i:
            to(send_ref.at[i], back_ref.at[col], send_sem.at[i], back_sem.at[col], {"ep": col}).wait_recv()
        local = cols + col * blk_rows
        hit = (slot_ref[:, 0:1] == local) | (slot_ref[:, 1:2] == local)
        acc += mm(one_hot(hit), back_ref[col])
        if k == 1:
            for copy in col_copies.values():
                copy.start()
    out_ref[...] = acc

    col_part[o] = col_sum[...]
    for i in range(1, n_ep):
        col = col_at(i)
        to(col_sum, col_part.at[col], col_sem.at[0, i], col_sem.at[1, col], {"ep": col}).wait_recv()
    total = col_part[0]
    for k in range(1, n_ep):
        total += col_part[k]
    total_ref[...] = total
    for copy in [*z_copies, *copies.values(), *col_copies.values()]:
        copy.wait_send()


def return_rows(starts, near, far, more, part, slots, n_etp, n_ep, blk_rows):
    d_model = near.shape[1]
    out = jax.ShapeDtypeStruct((slots.shape[0], d_model), F32)
    dma = pltpu.SemaphoreType.DMA
    vmem = lambda array: rows_at(*array.shape)
    blocks = pltpu.VMEM((n_ep, blk_rows, d_model), BF16)
    return pl.pallas_call(
        functools.partial(return_kernel, n_etp),
        grid=(1,),
        in_specs=[pl.BlockSpec(memory_space=pltpu.SMEM), vmem(near), vmem(far), vmem(more), vmem(part), vmem(slots)],
        out_specs=[vmem(out), vmem(part)],
        out_shape=[out, jax.ShapeDtypeStruct(part.shape, F32)],
        scratch_shapes=[
            pltpu.VMEM((near.shape[0] + more.shape[0], d_model), BF16),
            blocks,
            blocks,
            pltpu.VMEM((n_etp, *part.shape), F32),
            pltpu.VMEM((n_ep, *part.shape), F32),
            pltpu.VMEM(part.shape, F32),
            dma((n_ep,)),
            dma((n_ep,)),
            dma((2, n_etp)),
            dma((2, n_ep)),
        ],
        compiler_params=pltpu.CompilerParams(collective_id=1, has_side_effects=True, vmem_limit_bytes=42 * MIB),
        cost_estimate=cost(10**10, 12 * near.size),
        name="return_rows",
    )(starts, near, far, more, part, slots)


def split3(value):
    high = lax.reduce_precision(value, 8, 7)
    rest = value - high
    mid = lax.reduce_precision(rest, 8, 7)
    return high.astype(BF16), mid.astype(BF16), (rest - mid).astype(BF16)


def solution(mesh):
    ep_size = mesh.shape["ep"]
    etp_size = mesh.shape["etp"]
    n_dev = ep_size * etp_size
    tok_spec = P(ALL_AXES, None)
    gate_spec = P("ep", None, "etp")
    down_spec = P("ep", "etp", None)

    def layer(hidden, w_router, expert_ids, d_out, w_gate, w_up, w_down):
        tok_rows, d_model = hidden.shape
        n_experts = w_router.shape[1]
        n_tokens = tok_rows * n_dev
        capacity = (5 * n_tokens + 2 * n_experts - 1) // (2 * n_experts)
        per_expert = 7 * tok_rows // (2 * n_experts)
        list_max = ep_size * per_expert
        main_rows = 23 * tok_rows // 8
        more_rows = list_max - main_rows
        tile = main_rows // 4
        win = per_expert + 8
        ep_i = lax.axis_index("ep")
        etp_i = lax.axis_index("etp")
        block_idx = ep_i * etp_size + etp_i
        w1, w3, w2 = w_gate[0], w_up[0], w_down[0]

        def swap(array, even, odd):
            pairs = [(t * ep_size + o, (odd if o % 2 else even)[t] * ep_size + o) for t in range(etp_size) for o in range(ep_size)]
            return lax.ppermute(array, ("etp", "ep"), pairs)

        ids_row = expert_ids.T.astype(BF16).reshape(1, 2 * tok_rows)
        ids_row = jnp.concatenate([ids_row, jnp.zeros((7, 2 * tok_rows), BF16)])
        h_all, dy_col = spread_all(jnp.concatenate([hidden, ids_row]), d_out, etp_size, ep_size)
        w1_b, w3_b, w2_b, h_all, dy_b = lax.optimization_barrier((w1, w3, w2, h_all, dy_col))
        w1p = swap(w1_b, NEXT_PAIRS, ENDS_PAIRS)
        w3p = swap(w3_b, NEXT_PAIRS, ENDS_PAIRS)
        w2p = swap(w2_b, NEXT_PAIRS, ENDS_PAIRS)

        def flip(array, bit):
            return lax.ppermute(array, "ep", [(o, o ^ bit) for o in range(ep_size)])

        half_z = etp_size // 2
        dy_c, dy_x, dy_y = [flip(dy_b, bit) for bit in (1, 2, 4)]
        dy_d = flip(dy_y[:half_z], 2), flip(dy_x[half_z:], 4)
        dy_cx, dy_cy = flip(dy_x, 1), flip(dy_y, 1)
        dy_d = jnp.concatenate(dy_d)
        dy_cd = flip(dy_d, 1)
        dy_all = [dy_b, dy_c, dy_x, dy_cx, dy_y, dy_cy, dy_d, dy_cd]
        dy_cols = (ep_i ^ jnp.arange(ep_size)).astype(jnp.int32)
        all_cols = jnp.arange(ep_size, dtype=jnp.int32)

        ids_all = h_all[:, tok_rows, :].astype(jnp.int32).reshape(n_dev, 2, tok_rows)
        id0, id1 = ids_all[:, 0], ids_all[:, 1]
        experts = jnp.arange(n_experts, dtype=jnp.int32)[None, :, None]
        count = jnp.sum(((id0[:, None, :] == experts) | (id1[:, None, :] == experts)).astype(F32), axis=2)
        before = jnp.cumsum(count, axis=0) - count
        kept = jnp.clip(capacity - before, 0, count).astype(jnp.int32)
        kept_lists = kept.reshape(ep_size, etp_size, n_experts)
        list_start = jnp.cumsum(kept_lists, axis=0) - kept_lists
        list_len = jnp.sum(kept_lists, axis=0)
        earlier = (jnp.arange(tok_rows)[:, None] < jnp.arange(tok_rows)[None, :]).astype(BF16)

        my_member = (id0 == ep_i) | (id1 == ep_i)
        my_rank = mm(my_member.astype(BF16), earlier).astype(jnp.int32)
        my_start = lax.dynamic_index_in_dim(list_start, ep_i, 2, keepdims=False)
        my_kept = lax.dynamic_index_in_dim(kept, ep_i, 1, keepdims=True)
        my_pos = jnp.where(my_member & (my_rank < my_kept), my_start.reshape(n_dev, 1) + my_rank, -1)
        odd = ep_i % 2
        far = jnp.where(odd == 1, etp_i ^ 1, etp_size - 1 - etp_i)
        planes = jnp.stack([far, etp_i, far ^ 2, etp_i ^ 2]).astype(jnp.int32)
        my_base = jnp.minimum(my_start, main_rows) // 8 * 8
        pick = functools.partial(pick_rows, win=win, n_src=ep_size, n_etp=etp_size)
        main_pos = jnp.where(my_pos < main_rows, my_pos, -1)
        main_base = my_base.T[planes]
        x_main = pick([h_all], all_cols, main_pos, None, planes, main_base, main_rows)

        route_w = jnp.concatenate(split3(w_router), axis=1)
        logit_parts = lax.dot_general(route_w, h_all, (((0,), (2,)), ((), ())), preferred_element_type=F32)[:, :, :tok_rows].reshape(-1, n_tokens)
        logits = logit_parts[:n_experts] + logit_parts[n_experts : 2 * n_experts] + logit_parts[2 * n_experts :]
        probs_all = jax.nn.softmax(logits, axis=0)
        expert_col = jnp.arange(n_experts, dtype=jnp.int32)[:, None]
        picked_all = jnp.where((id0.reshape(1, -1) == expert_col) | (id1.reshape(1, -1) == expert_col), probs_all, 0.0)
        my_gate = lax.dynamic_index_in_dim(picked_all, ep_i, 0, keepdims=False) / jnp.sum(picked_all, axis=0)
        mean_prob = jnp.sum(probs_all, axis=1) / n_tokens
        my_scale = OUT_SCALE * my_gate.reshape(n_dev, tok_rows)
        c_main = pick(dy_all, dy_cols, main_pos, my_scale, planes, main_base, main_rows)

        n_rows = x_main.shape[0]
        *acts, y_base = ffn_act(x_main, (w1, w3, w2), tile, 0, 8, (), n_rows)
        act_a, act_b, inner = ffn_act(x_main, (w1, w3), tile, 8, 8, acts, n_rows)
        far_a, far_b, far_u = ffn_act(x_main, (w1p, w3p), tile, 0, 4, (), main_rows)
        *grads, dx_base = ffn_grad(c_main, act_a, act_b, (w2, w1, w3), tile, 0, 0, 4, (), n_rows)
        y_far = []
        for i, n_tiles in enumerate((1, 3)):
            y_part = ffn_down(far_u, w2p, y_base, tile, i, n_tiles)
            y_far.append(swap(y_part, ENDS_PAIRS, NEXT_PAIRS))
        (dx_part,) = ffn_grad(c_main, far_a, far_b, (w2p, w1p, w3p), tile, 0, 0, 4, (), base=(dx_base,))
        dx_far = swap(dx_part, ENDS_PAIRS, NEXT_PAIRS)
        *grads, dx_base = ffn_grad(c_main, act_a, act_b, (w2, w1, w3), tile, 4, 4, 4, grads, n_rows)
        y_near, dx_near = ffn_pair(x_main, c_main, y_base, dx_base, (w1p, w3p, w2p), tile, 4, 4, 0)
        d_a, d_b = ffn_grad(c_main, act_a, act_b, (w2,), tile, 8, 8, 8, grads, n_rows)

        def add_planes(parts):
            total = parts[etp_i]
            for k in range(1, etp_size):
                shift = [(t, (t + k) % etp_size) for t in range(etp_size)]
                total += lax.ppermute(parts[(etp_i + k) % etp_size], "etp", shift)
            return total

        def more_work(*_):
            more_pos = jnp.where(my_pos >= main_rows, my_pos - main_rows, -1)
            more_base = jnp.clip(my_start.T - main_rows, 0, more_rows) // 8 * 8
            order = jnp.arange(etp_size, dtype=jnp.int32)
            x_more = pick([h_all], all_cols, more_pos, None, order, more_base, more_rows)
            c_more = pick(dy_all, dy_cols, more_pos, my_scale, order, more_base, more_rows)
            act_a, act_b, inner, y_part = ffn_act(x_more, (w1, w3, w2), more_rows, 0, etp_size, (), n_more)
            d_a, d_b, dx_part = ffn_grad(c_more, act_a, act_b, (w2, w1, w3), more_rows, 0, 0, etp_size, (), n_more)
            sums = [add_planes(part.reshape(etp_size, more_rows, d_model)).astype(BF16) for part in (y_part, dx_part)]
            return *sums, x_more, c_more, inner, d_a, d_b

        n_more = etp_size * more_rows
        none = jnp.zeros((more_rows, d_model), BF16)
        spare = none, none, *unset(*[(n_more, d_model)] * 2, *[(n_more, w1.shape[1])] * 3)
        any_more = jnp.max(list_len) > main_rows
        y_more, dx_more, x_more, c_more, *more_acts = lax.cond(any_more, more_work, lambda *spare: spare, *spare)

        def more_grads(*grads):
            inner_more, d_a_more, d_b_more = more_acts
            return grads[0] + mm_tn(x_more, d_a_more), grads[1] + mm_tn(x_more, d_b_more), grads[2] + mm_tn(inner_more, c_more)

        home_start = lax.dynamic_index_in_dim(my_start, etp_i, 1, keepdims=False)

        hot = [(expert_ids[:, k : k + 1] == experts[0].T).astype(F32) for k in range(2)]
        probs = lax.dynamic_slice_in_dim(probs_all, block_idx * tok_rows, tok_rows, 1).T
        picked = [jnp.sum(probs * hot[k], axis=1, keepdims=True) for k in range(2)]
        pick_sum = picked[0] + picked[1]
        gates = [picked[k] / pick_sum for k in range(2)]
        my_kept_row = lax.dynamic_index_in_dim(kept, block_idx, 0, keepdims=True).astype(F32)
        rank = mm_tn(earlier, (hot[0] + hot[1]).astype(BF16))
        slot_row = jnp.arange(n_experts * per_expert, dtype=jnp.int32)[None, :]
        slots, chosen = [], []
        for k in range(2):
            rank_k = jnp.sum(rank * hot[k], axis=1, keepdims=True)
            kept_k = jnp.sum(my_kept_row * hot[k], axis=1, keepdims=True)
            slot_k = jnp.where(rank_k < kept_k, expert_ids[:, k : k + 1] * per_expert + rank_k.astype(jnp.int32), -1)
            slots.append(slot_k)
            chosen.append(slot_k == slot_row)

        dw1 = mm_tn(x_main, d_a)
        y_near, dw1, x_main = lax.optimization_barrier((y_near, dw1, x_main))
        y_back = home_blocks(home_start, y_near, y_far, y_more, per_expert)
        y_back = lax.all_to_all(y_back, "ep", 0, 0, tiled=True).reshape(n_experts * per_expert, d_model)
        dw3 = mm_tn(x_main, d_b)
        dw2 = mm_tn(inner, c_main)
        dw1, dw3, dw2 = lax.cond(any_more, more_grads, lambda *grads: grads, dw1, dw3, dw2)
        y_pair = [mm(chosen[k].astype(BF16), y_back) for k in range(2)]
        hidden_f = hidden.astype(F32)
        output = (hidden_f + OUT_SCALE * (gates[0] * y_pair[0] + gates[1] * y_pair[1])).astype(BF16)
        d_out_f = d_out.astype(F32)
        d_gates = [jnp.sum(OUT_SCALE * d_out_f * y_pair[k], axis=1, keepdims=True) for k in range(2)]

        route_frac = jnp.sum(count, axis=0) / (2 * n_tokens)
        aux_loss = AUX_COEF * n_experts * jnp.sum(route_frac * mean_prob)
        mix = gates[0] * d_gates[0] + gates[1] * d_gates[1]
        d_probs = (AUX_COEF * n_experts / n_tokens) * route_frac[None, :]
        for k in range(2):
            d_probs = d_probs + hot[k] * ((d_gates[k] - mix) / pick_sum)
        d_logits = probs * (d_probs - jnp.sum(probs * d_probs, axis=1, keepdims=True))
        d_router_part = mm_tn(d_logits, hidden_f, lax.Precision.HIGHEST)
        d_route = mm_nt(d_logits, w_router, lax.Precision.HIGHEST)
        rest = d_out_f + d_route
        dx_near, dw1, dw3, dw2, rest, output = lax.optimization_barrier((dx_near, dw1, dw3, dw2, rest, output))
        dx_sum, d_router = return_rows(home_start, dx_near, dx_far, dx_more, d_router_part, jnp.concatenate(slots, axis=1), etp_size, ep_size, per_expert)
        d_hidden = (rest + dx_sum).astype(BF16)
        d_router = d_router.T
        return output, d_hidden, d_router, aux_loss, dw1[None], dw3[None], dw2[None]

    return jax.shard_map(layer, mesh=mesh, in_specs=(tok_spec, P(), tok_spec, tok_spec, gate_spec, gate_spec, down_spec), out_specs=(tok_spec, tok_spec, P(), P(), gate_spec, gate_spec, down_spec), check_vma=False)
```
